32 devices in a mesh: grp: 2 (over x), seq: 16 (over z, y, core).
Axes of the slice: x: 2, y: 2, z: 4, core: 2. Of those that a mesh axis runs over, the one named last changes fastest.
Arguments:
- cont_query: bfloat16 [64, 32, 2560], P(('grp', 'seq')), parts along dimension 0, may hold values from -180 to 180
- cont_key: bfloat16 [64, 32, 512], P(('grp', 'seq')), parts along dimension 0, may hold values from -6 to 6
- cont_value: bfloat16 [64, 32, 512], P(('grp', 'seq')), parts along dimension 0, may hold values from -6 to 6
- prefix_key: bfloat16 [4, 2048, 512], P('grp', 'seq'), parts along dimension 0, may hold values from -7 to 7
- prefix_value: bfloat16 [4, 2048, 512], P('grp', 'seq'), parts along dimension 0, may hold values from -6 to 6
- out_weight: bfloat16 [2560, 2560], P(None, 'seq'), may hold values from -0.125 to 0.125
- norm_gain: float32 [2560], replicated, may hold values from 0.5 to 1.5
- lm_head: bfloat16 [2560, 76032], P(None, 'seq'), may hold values from -18 to 18
- target_ids: int32 [64, 32], P(('grp', 'seq')), parts along dimension 0, may hold values from 0 to 76031
- cont_len: int32 [64], P(('grp', 'seq')), parts along dimension 0, may hold values from 8 to 32
- prompt_len: int32 [4], P('grp'), parts along dimension 0, may hold values from 1024 to 2048
- group_of: int32 [64], P('grp'), parts along dimension 0, may hold values from 0 to 1, as said below
- rewards: float32 [64], P(('grp', 'seq')), parts along dimension 0, may hold values from -13 to 13
Outputs:
- token_logprob: float32 [64, 32], P(('grp', 'seq')), parts along dimension 0
- advantage: float32 [64], P(('grp', 'seq')), parts along dimension 0
- objective: float32 [64], P(('grp', 'seq')), parts along dimension 0
The draws below stay inside these ranges and needn't reach their ends.
There are 2 independent parts, one for each index of `grp`. The reference program is written for one: setup_inputs(seed, part) draws one part's arguments, and reference() takes and returns one part's arrays. A program takes and returns all parts, laid end to end along the dimension named above; an argument that names none is the same for every part. Nothing has to cross between parts.
Inputs may be any that keep to these rules, and one draw needn't show every extreme that they name: `group_of`: each of the 2 prompts is named by exactly 16 continuations.
All inputs are finite; a program needn't handle non-finite values.
Results may differ from the reference program's by a relative error of at most 0.0026.
Values may be sent and summed in bfloat16 or wider, within the bound.
A program may use at most 128 MiB of HBM per device.

```python
import math
import jax
import jax.numpy as jnp
import numpy as np
from jax import lax

D = 2560
QH = 20
KVH = 4
HD = 128
VOCAB = 76032
GROUP = 16
CLEN = 32
PROMPT = 2048
CONTS = 32
PROMPTS = 2
N_SEQ = 16


def draw_groups(key):
    shuffled = jax.random.permutation(jax.random.fold_in(key, 11), CONTS)
    return (shuffled // GROUP).astype(jnp.int32)


def draw_group_of(key, part):
    return draw_groups(key)


def draw_prefix_key(key, part):
    drawn = jnp.clip(jax.random.normal(jax.random.fold_in(key, 13), (PROMPTS, PROMPT, KVH * HD), jnp.float32), -6.0, 6.0)
    return drawn.astype(jnp.bfloat16)


def draw_cont_query(key, part):
    drawn = jnp.clip(jax.random.normal(jax.random.fold_in(key, 14), (CONTS, CLEN, QH * HD), jnp.float32), -6.0, 6.0)
    return drawn.astype(jnp.bfloat16)


def draw_lm_head(key, part):
    drawn = jnp.clip(jax.random.normal(jax.random.fold_in(key, 19), (D, VOCAB), jnp.float32), -6.0, 6.0)
    column_scale = jnp.full((1, VOCAB), 3.0 / math.sqrt(D), jnp.float32)
    return (drawn * column_scale).astype(jnp.bfloat16)


def draw_rewards(key, part):
    groups = draw_groups(key)
    spread = jnp.exp(jax.random.uniform(jax.random.fold_in(key, 16), (PROMPTS,), jnp.float32, math.log(0.05), math.log(2.0)))
    offset = jax.random.uniform(jax.random.fold_in(key, 17), (PROMPTS,), jnp.float32, -1.0, 1.0)
    jitter = jnp.clip(jax.random.normal(jax.random.fold_in(key, 18), (CONTS,), jnp.float32), -6.0, 6.0)
    return offset[groups] + spread[groups] * jitter


def place_ends(array, own_key, smallest, largest):
    shape = array.shape
    index_at = [jax.random.randint(jax.random.fold_in(own_key, axis), (), 0, shape[axis]) for axis in range(len(shape))]
    array = array.at[tuple(index_at)].set(smallest)
    longest = shape.index(max(shape))
    index_at[longest] = (index_at[longest] + 1) % shape[longest]
    return array.at[tuple(index_at)].set(largest)


def level_of(stream_key, dims, pieces, least, largest):
    factor_of = 1.0
    for axis_at, blocks in pieces:
        draws = jax.random.uniform(jax.random.fold_in(jax.random.fold_in(stream_key, 6), axis_at), (blocks,), jnp.float32, least / len(pieces), largest / len(pieces))
        factor_of = factor_of * jnp.repeat(jnp.exp(draws), dims[axis_at] // blocks).reshape((-1,) + (1,) * (len(dims) - 1 - axis_at))
    return factor_of


def skewed_wide(stream_key, dims, number_of, lean):
    loads = [min(1 << octave, number_of + 1 - (1 << octave)) * (1 << 20) // math.isqrt((1 << octave) ** lean) + 1 for octave in range((number_of + 1).bit_length()) if 1 << octave <= number_of]
    width = 1 + sum(loads) // (1 << 30)
    listing = np.cumsum(np.array([max(1, weight // width) for weight in loads]))
    ticket = jax.random.randint(jax.random.fold_in(stream_key, 1), dims, 0, int(listing[len(loads) - 1]))
    start = jnp.left_shift(1, jnp.searchsorted(jnp.asarray(listing, jnp.int32), ticket, side="right").astype(jnp.int32))
    grade = start - 1 + jax.random.randint(jax.random.fold_in(stream_key, 4), dims, 0, 1 << 30) % jnp.minimum(start, number_of + 1 - start)
    return jax.random.permutation(jax.random.fold_in(stream_key, 2), number_of)[grade].astype(jnp.int32)


def bell_draw(own_key, shape, scale, bound, shards=(), held_as=jnp.bfloat16):
    values = scale * jax.random.normal(own_key, shape, jnp.float32)
    if shards:
        values = values * level_of(own_key, shape, shards, -0.22, 0.18)
    return jnp.clip(values, -bound, bound).astype(held_as)


def setup_inputs(seed: int = 0, part: int = 0) -> dict:
    key_list = jax.random.split(jax.random.key(seed), 14)
    part_keys = jax.random.split(jax.random.fold_in(key_list[13], part), 14)
    return {
        "cont_query": draw_cont_query(jax.random.fold_in(jax.random.fold_in(key_list[13], part), 71), part),
        "cont_key": bell_draw(part_keys[1], (CONTS, CLEN, KVH * HD), 1.0, 6.0, ((0, 16),)),
        "cont_value": bell_draw(part_keys[2], (CONTS, CLEN, KVH * HD), 1.0, 6.0, ((0, 16),)),
        "prefix_key": draw_prefix_key(jax.random.fold_in(jax.random.fold_in(key_list[13], part), 71), part),
        "prefix_value": bell_draw(part_keys[4], (PROMPTS, PROMPT, KVH * HD), 1.0, 6.0, ((1, 16),)),
        "out_weight": bell_draw(key_list[5], (QH * HD, D), (QH * HD) ** -0.5, 0.125, ((1, 16),)),
        "norm_gain": jnp.clip(1.0 + 0.1 * jax.random.normal(key_list[6], (D,), jnp.float32), 0.5, 1.5),
        "lm_head": draw_lm_head(jax.random.fold_in(key_list[13], 71), part),
        "target_ids": place_ends(skewed_wide(part_keys[8], (CONTS, CLEN), VOCAB, 2), jax.random.fold_in(part_keys[8], 3), 0, VOCAB - 1).astype(jnp.int32),
        "cont_len": place_ends(jax.random.randint(part_keys[9], (CONTS,), CLEN // 4, CLEN + 1), jax.random.fold_in(part_keys[9], 1), CLEN // 4, CLEN).astype(jnp.int32),
        "prompt_len": jax.random.randint(part_keys[10], (PROMPTS,), PROMPT // 2, PROMPT + 1).astype(jnp.int32),
        "group_of": draw_group_of(jax.random.fold_in(jax.random.fold_in(key_list[13], part), 71), part),
        "rewards": draw_rewards(jax.random.fold_in(jax.random.fold_in(key_list[13], part), 71), part),
    }


NEGATIVE = -1e+30
EPSILON = 1e-06
REWARD_FLOOR = 0.25

def normalize(hidden, norm_gain):
    widened = hidden.astype(jnp.float32)
    factor = lax.rsqrt(lax.optimization_barrier(jnp.mean(widened * widened, axis=-1, keepdims=True)) + EPSILON)
    return (widened * factor * norm_gain).astype(jnp.bfloat16)

def shard_stats(normed, token_ids, head, vocab_offset):
    logits = jnp.dot(normed, head, preferred_element_type=jnp.float32)
    maximum = lax.optimization_barrier(jnp.max(logits, axis=1))
    total_mass = lax.optimization_barrier(jnp.sum(jnp.exp(logits - maximum[:, None]), axis=1))
    columns = vocab_offset + jnp.arange(head.shape[1], dtype=jnp.int32)
    picked = lax.optimization_barrier(jnp.sum(jnp.where(token_ids[:, None] == columns[None, :], logits, 0.0), axis=1))
    return (maximum, total_mass, picked)

def join_stats(first, second):
    maximum = jnp.maximum(first[0], second[0])
    total_mass = first[1] * jnp.exp(first[0] - maximum) + second[1] * jnp.exp(second[0] - maximum)
    return (maximum, total_mass, first[2] + second[2])

def reference(cont_query, cont_key, cont_value, prefix_key, prefix_value, out_weight, norm_gain, lm_head, target_ids, cont_len, prompt_len, group_of, rewards):
    per_group = QH // KVH
    position = jnp.arange(CLEN, dtype=jnp.int32)
    causal = position[None, :] <= position[:, None]
    highest = lax.Precision.HIGHEST

    def attend(index):
        prompt = group_of[index]
        key_rows = jnp.concatenate([prefix_key[prompt], cont_key[index]], axis=0).astype(jnp.float32).reshape(PROMPT + CLEN, KVH, HD)
        value_rows = jnp.concatenate([prefix_value[prompt], cont_value[index]], axis=0).astype(jnp.float32).reshape(PROMPT + CLEN, KVH, HD)
        queries = cont_query[index].astype(jnp.float32).reshape(CLEN, KVH, per_group, HD)
        scores = jnp.einsum('tkgd,skd->tkgs', queries, key_rows, precision=highest) * HD ** (-0.5)
        early = jnp.broadcast_to((jnp.arange(PROMPT, dtype=jnp.int32) < prompt_len[prompt])[None, :], (CLEN, PROMPT))
        visible = jnp.concatenate([early, causal], axis=1)[:, None, None, :]
        scores = jnp.where(visible, scores, NEGATIVE)
        maximum = lax.optimization_barrier(jnp.max(scores, axis=-1, keepdims=True))
        weights = jnp.where(visible, jnp.exp(scores - maximum), 0.0)
        total = lax.optimization_barrier(jnp.sum(weights, axis=-1))
        mixed = jnp.einsum('tkgs,skd->tkgd', weights, value_rows, precision=highest) / total[..., None]
        return mixed.astype(jnp.bfloat16).reshape(CLEN, QH * HD)
    attended = lax.map(attend, jnp.arange(CONTS, dtype=jnp.int32)).reshape(CONTS * CLEN, QH * HD)
    hidden = jnp.dot(attended, out_weight, preferred_element_type=jnp.float32).astype(jnp.bfloat16)
    normed = normalize(hidden, norm_gain)
    token_ids = target_ids.reshape(CONTS * CLEN)
    block = VOCAB // N_SEQ

    def vocab_step(step, running):
        head = lax.dynamic_slice_in_dim(lm_head, step * block, block, 1)
        stats = shard_stats(normed, token_ids, head, step * block)
        return join_stats(running, stats)
    start_stats = (jnp.full((CONTS * CLEN,), NEGATIVE, jnp.float32), jnp.zeros((CONTS * CLEN,), jnp.float32), jnp.zeros((CONTS * CLEN,), jnp.float32))
    maximum, total_mass, picked = lax.fori_loop(0, N_SEQ, vocab_step, start_stats)
    logprob = (picked - maximum - jnp.log(total_mass)).reshape(CONTS, CLEN)
    live = position[None, :] < cont_len[:, None]
    token_logprob = jnp.where(live, logprob, 0.0)
    same_group = (group_of[:, None] == group_of[None, :]).astype(jnp.float32)
    group_mean = jnp.dot(same_group, rewards, precision=highest) / GROUP
    deviation = rewards[None, :] - group_mean[:, None]
    spread = jnp.sqrt(lax.optimization_barrier(jnp.sum(same_group * deviation * deviation, axis=1)) / (GROUP - 1))
    advantage = (rewards - group_mean) / jnp.maximum(spread, REWARD_FLOOR)
    objective = advantage * lax.optimization_barrier(jnp.sum(token_logprob, axis=1)) / cont_len.astype(jnp.float32)
    return (token_logprob, advantage, objective)
```

```python
import functools

import jax
import jax.numpy as jnp
from jax import lax
from jax.experimental import pallas as pl
from jax.experimental.pallas import tpu as pltpu
from jax.sharding import PartitionSpec as P

HD = 128
GROUP = 16
NEGATIVE = -1e30
EPSILON = 1e-06
REWARD_FLOOR = 0.25
MESH = pl.DeviceIdType.MESH
VMEM = pltpu.VMEM
LIMIT = 60 * 1024 * 1024


class Place:
    def __init__(self, n, planes):
        self.n, self.planes = n, planes
        self.lanes = n // planes
        self.half = self.lanes // 2
        self.me = lax.axis_index("seq")
        self.plane = self.me // self.lanes
        lane = self.me % self.lanes
        self.row = lane // 2
        self.core = lane % 2

    def device(self, plane, row, core):
        return plane * self.lanes + row * 2 + core

    def plane_at(self, step):
        return (self.plane + step) % self.planes

    def row_at(self, step):
        return (self.row + step) % self.half

    def peers(self):
        out = [self.device(self.plane_at(d), self.row, self.core) for d in range(1, self.planes)]
        out += [self.device(self.plane, self.row_at(e), self.core) for e in range(1, self.half)]
        return out + [self.device(self.plane, self.row, 1 - self.core)]


def greet(peers):
    barrier = pltpu.get_barrier_semaphore()
    for peer in peers:
        pl.semaphore_signal(barrier, inc=1, device_id={"seq": peer}, device_id_type=MESH)
    pl.semaphore_wait(barrier, len(peers))


def send_count(n, planes):
    half = n // planes // 2
    return (planes - 1) + half + (planes - 1) * half + planes * (half - 1)


class Spread:
    def __init__(self, at, parts, own, full, send_sem, recv_sem, local_sem):
        self.at, self.parts, self.own, self.full = at, parts, own, full
        self.send_sem, self.recv_sem, self.local_sem = send_sem, recv_sem, local_sem
        self.sent = []

    def send(self, src_ref, source, part, target):
        copy = pltpu.make_async_remote_copy(
            src_ref=src_ref,
            dst_ref=self.full(source, part),
            send_sem=self.send_sem.at[len(self.sent)],
            recv_sem=self.recv_sem.at[source * self.parts + part],
            device_id={"seq": target},
            device_id_type=MESH,
        )
        copy.start()
        self.sent.append(copy)

    def arrived(self, source, part):
        pltpu.make_async_remote_copy(
            src_ref=self.full(source, part),
            dst_ref=self.full(source, part),
            send_sem=self.send_sem.at[0],
            recv_sem=self.recv_sem.at[source * self.parts + part],
            device_id={"seq": self.at.device(self.at.plane, self.at.row, 1 - self.at.core)},
            device_id_type=MESH,
        ).wait_recv()

    def to_rows(self, src_ref, source, part):
        at = self.at
        for e in range(1, at.half):
            self.send(src_ref, source, part, at.device(at.plane, at.row_at(e), at.core))

    def to_core(self, src_ref, source, part):
        at = self.at
        self.send(src_ref, source, part, at.device(at.plane, at.row, 1 - at.core))

    def start(self):
        at = self.at
        self.local = []
        for part in range(self.parts):
            for d in range(1, at.planes):
                target = at.plane_at(d)
                self.send(
                    self.own(part, target), at.me, part, at.device(target, at.row, at.core)
                )
            self.to_rows(self.own(part, at.plane), at.me, part)
            self.to_core(self.own(part, at.plane), at.me, part)
            copy = pltpu.make_async_copy(
                self.own(part, at.plane), self.full(at.me, part), self.local_sem.at[part]
            )
            copy.start()
            self.local.append(copy)

    def from_rows(self, plane):
        at = self.at
        for part in range(self.parts):
            for e in range(1, at.half):
                source = at.device(plane, at.row_at(e), at.core)
                self.arrived(source, part)
                self.to_core(self.full(source, part), source, part)

    def from_plane(self, plane):
        at = self.at
        for part in range(self.parts):
            source = at.device(plane, at.row, at.core)
            self.arrived(source, part)
            self.to_rows(self.full(source, part), source, part)
            self.to_core(self.full(source, part), source, part)

    def finish(self):
        at = self.at
        order = [at.plane_at(d) for d in [1, at.planes - 1] + list(range(2, at.planes - 1))]
        self.from_rows(at.plane)
        for i, plane in enumerate(order):
            self.from_plane(plane)
            if i >= 1:
                self.from_rows(order[i - 1])
        self.from_rows(order[-1])
        for plane in range(at.planes):
            for row in range(at.half):
                for part in range(self.parts):
                    self.arrived(at.device(plane, row, 1 - at.core), part)
        for copy in self.sent:
            copy.wait_send()
        for copy in self.local:
            copy.wait()


def exchange_kernel(
    n,
    planes,
    q_ref,
    ck_ref,
    cv_ref,
    pk_ref,
    pv_ref,
    meta_ref,
    q_out,
    ck_out,
    cv_out,
    pk_out,
    pv_out,
    meta_out,
    send_sem,
    recv_sem,
    local_sem,
    lane_send,
    lane_recv,
    lane_local,
    meta_send,
    meta_recv,
    meta_local,
):
    at = Place(n, planes)
    greet([(at.me + d) % n for d in range(1, n)])
    conts = q_ref.shape[0]
    span = pk_ref.shape[1]

    def head(ref, plane):
        width = ref.shape[2] // planes
        return ref.at[:, :, pl.ds(pl.multiple_of(plane * width, 128), width)]

    def own(part, plane):
        return head((pk_ref, pv_ref)[part], plane)

    def full(source, part):
        start = pl.multiple_of(source * span, 128)
        return (pk_out, pv_out)[part].at[:, pl.ds(start, span), :]

    spread = Spread(at, 2, own, full, send_sem, recv_sem, local_sem)
    spread.start()
    pairs = ((q_ref, q_out), (ck_ref, ck_out), (cv_ref, cv_out))
    waits = []
    for i, (src, dst) in enumerate(pairs):
        mine = dst.at[pl.ds(at.plane * conts, conts)]
        for d in range(1, planes):
            target = at.plane_at(d)
            copy = pltpu.make_async_remote_copy(
                src_ref=head(src, target),
                dst_ref=mine,
                send_sem=lane_send.at[i * planes + d],
                recv_sem=lane_recv.at[i * planes + at.plane],
                device_id={"seq": at.device(target, at.row, at.core)},
                device_id_type=MESH,
            )
            copy.start()
            waits.append(copy.wait_send)
        copy = pltpu.make_async_copy(head(src, at.plane), mine, lane_local.at[i])
        copy.start()
        waits.append(copy.wait)
    for d in range(1, n):
        copy = pltpu.make_async_remote_copy(
            src_ref=meta_ref,
            dst_ref=meta_out.at[at.me],
            send_sem=meta_send.at[d],
            recv_sem=meta_recv.at[at.me],
            device_id={"seq": (at.me + d) % n},
            device_id_type=MESH,
        )
        copy.start()
        waits.append(copy.wait_send)
    copy = pltpu.make_async_copy(meta_ref, meta_out.at[at.me], meta_local)
    copy.start()
    waits.append(copy.wait)
    spread.finish()
    for i, (src, dst) in enumerate(pairs):
        for d in range(1, planes):
            source = at.plane_at(d)
            landed = dst.at[pl.ds(source * conts, conts)]
            pltpu.make_async_remote_copy(
                src_ref=landed,
                dst_ref=landed,
                send_sem=lane_send.at[i * planes + d],
                recv_sem=lane_recv.at[i * planes + source],
                device_id={"seq": at.device(source, at.row, at.core)},
                device_id_type=MESH,
            ).wait_recv()
    for d in range(1, n):
        source = (at.me + d) % n
        pltpu.make_async_remote_copy(
            src_ref=meta_ref,
            dst_ref=meta_out.at[source],
            send_sem=meta_send.at[d],
            recv_sem=meta_recv.at[source],
            device_id={"seq": source},
            device_id_type=MESH,
        ).wait_recv()
    for wait in waits:
        wait()


def exchange(n, planes, q, ck, cv, pk, pv, meta):
    conts, steps, width = q.shape
    prompts, span, _ = pk.shape
    dma = pltpu.SemaphoreType.DMA
    shape = jax.ShapeDtypeStruct
    return pl.pallas_call(
        functools.partial(exchange_kernel, n, planes),
        out_shape=(
            shape((conts * planes, steps, width // planes), q.dtype),
            shape((conts * planes, steps, ck.shape[2] // planes), q.dtype),
            shape((conts * planes, steps, ck.shape[2] // planes), q.dtype),
            shape((prompts, span * n, pk.shape[2] // planes), q.dtype),
            shape((prompts, span * n, pk.shape[2] // planes), q.dtype),
            shape((n,) + meta.shape, meta.dtype),
        ),
        in_specs=[pl.BlockSpec(memory_space=VMEM)] * 6,
        out_specs=(pl.BlockSpec(memory_space=VMEM),) * 6,
        scratch_shapes=[
            dma((2 * send_count(n, planes),)),
            dma((2 * n,)),
            dma((2,)),
            dma((3 * planes,)),
            dma((3 * planes,)),
            dma((3,)),
            dma((n,)),
            dma((n,)),
            dma,
        ],
        compiler_params=pltpu.CompilerParams(
            collective_id=0, has_side_effects=True, vmem_limit_bytes=LIMIT
        ),
        name="exchange",
    )(q, ck, cv, pk, pv, meta)


def attention_kernel(group_ref, length_ref, q_ref, ck_ref, cv_ref, pk_ref, pv_ref, out_ref):
    cont = pl.program_id(0)
    prompt = group_ref[cont]
    length = length_ref[prompt]
    steps, width = q_ref.shape[1:]
    heads = width // HD
    q = q_ref[0]
    rows = jnp.concatenate([q[:, h * HD : (h + 1) * HD] for h in range(heads)], axis=0)
    contract = (((1,), (1,)), ((), ()))
    early = lax.dot_general(rows, pk_ref[prompt], contract, preferred_element_type=jnp.float32)
    late = lax.dot_general(rows, ck_ref[0], contract, preferred_element_type=jnp.float32)
    scale = HD ** (-0.5)
    column = lax.broadcasted_iota(jnp.int32, early.shape, 1)
    early = jnp.where(column < length, early * scale, NEGATIVE)
    line = lax.broadcasted_iota(jnp.int32, late.shape, 0) % steps
    late = jnp.where(
        lax.broadcasted_iota(jnp.int32, late.shape, 1) <= line, late * scale, NEGATIVE
    )
    peak = jnp.maximum(
        jnp.max(early, axis=1, keepdims=True), jnp.max(late, axis=1, keepdims=True)
    )
    early = jnp.exp(early - peak).astype(jnp.bfloat16)
    late = jnp.exp(late - peak).astype(jnp.bfloat16)
    total = jnp.sum(early.astype(jnp.float32), axis=1, keepdims=True) + jnp.sum(
        late.astype(jnp.float32), axis=1, keepdims=True
    )
    mixed = jnp.dot(early, pv_ref[prompt], preferred_element_type=jnp.float32) + jnp.dot(
        late, cv_ref[0], preferred_element_type=jnp.float32
    )
    mixed = (mixed / total).astype(jnp.bfloat16)
    out_ref[...] = jnp.concatenate(
        [mixed[h * steps : (h + 1) * steps] for h in range(heads)], axis=1
    )


def attention(groups, lengths, q, ck, cv, pk, pv):
    conts, steps, width = q.shape
    whole = pl.BlockSpec(memory_space=VMEM)
    scalar = pl.BlockSpec(memory_space=pltpu.SMEM)
    return pl.pallas_call(
        attention_kernel,
        out_shape=jax.ShapeDtypeStruct((conts * steps, width), jnp.bfloat16),
        grid=(conts,),
        in_specs=[
            scalar,
            scalar,
            pl.BlockSpec((1, steps, width), lambda c: (c, 0, 0)),
            pl.BlockSpec((1, steps, ck.shape[2]), lambda c: (c, 0, 0)),
            pl.BlockSpec((1, steps, ck.shape[2]), lambda c: (c, 0, 0)),
            whole,
            whole,
        ],
        out_specs=pl.BlockSpec((steps, width), lambda c: (c, 0)),
        compiler_params=pltpu.CompilerParams(vmem_limit_bytes=LIMIT),
        name="attention",
    )(groups, lengths, q, ck, cv, pk, pv)


PARTS = 2


def tokens_kernel(n, planes, x_ref, out_ref, send_sem, recv_sem, local_sem):
    at = Place(n, planes)
    greet(at.peers())
    rows, width = x_ref.shape
    piece = rows // PARTS

    def own(part, plane):
        return x_ref.at[pl.ds(part * piece, piece)]

    def full(source, part):
        start = pl.multiple_of(source % at.lanes * rows + part * piece, 16)
        column = pl.multiple_of(source // at.lanes * width, 128)
        return out_ref.at[pl.ds(start, piece), pl.ds(column, width)]

    spread = Spread(at, PARTS, own, full, send_sem, recv_sem, local_sem)
    spread.start()
    spread.finish()


def features_kernel(n, planes, x_ref, out_ref, send_sem, recv_sem, local_sem):
    at = Place(n, planes)
    greet(at.peers())
    rows, width = x_ref.shape
    piece = width // PARTS

    def own(part, plane):
        return x_ref.at[:, pl.ds(part * piece, piece)]

    def full(source, part):
        start = pl.multiple_of(source * rows, 16)
        return out_ref.at[pl.ds(start, rows), pl.ds(part * piece, piece)]

    spread = Spread(at, PARTS, own, full, send_sem, recv_sem, local_sem)
    spread.start()
    spread.finish()


def gather(kernel, n, planes, x, shape, number, name):
    dma = pltpu.SemaphoreType.DMA
    return pl.pallas_call(
        functools.partial(kernel, n, planes),
        out_shape=jax.ShapeDtypeStruct(shape, x.dtype),
        in_specs=[pl.BlockSpec(memory_space=VMEM)],
        out_specs=pl.BlockSpec(memory_space=VMEM),
        scratch_shapes=[
            dma((PARTS * send_count(n, planes),)),
            dma((PARTS * n,)),
            dma((PARTS,)),
        ],
        compiler_params=pltpu.CompilerParams(
            collective_id=number, has_side_effects=True, vmem_limit_bytes=LIMIT
        ),
        name=name,
    )(x)


TILE = 256


def logits_kernel(vocab, offset_ref, x_ref, ids_ref, head_ref, max_ref, sum_ref, pick_ref):
    step = pl.program_id(0)

    @pl.when(step == 0)
    def _():
        max_ref[...] = jnp.full_like(max_ref, NEGATIVE)
        sum_ref[...] = jnp.zeros_like(sum_ref)
        pick_ref[...] = jnp.zeros_like(pick_ref)

    logits = jnp.dot(x_ref[...], head_ref[...], preferred_element_type=jnp.float32)
    column = step * TILE + lax.broadcasted_iota(jnp.int32, (1, TILE), 1)
    wanted = ids_ref[...] - offset_ref[0]
    wanted = jnp.where(wanted < vocab, wanted, -1)
    logits = jnp.where(column < vocab, logits, NEGATIVE)
    best = max_ref[...]
    for at in range(0, TILE, 128):
        best = jnp.maximum(best, logits[:, at : at + 128])
    mass = sum_ref[...] * jnp.exp(max_ref[...] - best)
    pick = pick_ref[...]
    for at in range(0, TILE, 128):
        mass += jnp.exp(logits[:, at : at + 128] - best)
        pick += jnp.where(column[:, at : at + 128] == wanted, logits[:, at : at + 128], 0.0)
    max_ref[...] = best
    sum_ref[...] = mass
    pick_ref[...] = pick


def logit_stats(x, ids, head, offset):
    rows, depth = x.shape
    vocab = head.shape[1]
    whole = pl.BlockSpec((rows, 128), lambda v: (0, 0))
    return pl.pallas_call(
        functools.partial(logits_kernel, vocab),
        out_shape=(jax.ShapeDtypeStruct((rows, 128), jnp.float32),) * 3,
        grid=(pl.cdiv(vocab, TILE),),
        in_specs=[
            pl.BlockSpec(memory_space=pltpu.SMEM),
            pl.BlockSpec(memory_space=VMEM),
            pl.BlockSpec(memory_space=VMEM),
            pl.BlockSpec((depth, TILE), lambda v: (0, v)),
        ],
        out_specs=(whole,) * 3,
        compiler_params=pltpu.CompilerParams(vmem_limit_bytes=LIMIT),
        name="logits",
    )(offset, x, ids, head)


def stats_kernel(n, x_ref, out_ref, send_sem, recv_sem, local_sem):
    me = lax.axis_index("seq")
    greet([(me + d) % n for d in range(1, n)])
    sent = []
    for d in range(1, n):
        target = (me + d) % n
        copy = pltpu.make_async_remote_copy(
            src_ref=x_ref.at[target],
            dst_ref=out_ref.at[me],
            send_sem=send_sem.at[d],
            recv_sem=recv_sem.at[me],
            device_id={"seq": target},
            device_id_type=MESH,
        )
        copy.start()
        sent.append(copy)
    local = pltpu.make_async_copy(x_ref.at[me], out_ref.at[me], local_sem)
    local.start()
    for d in range(1, n):
        source = (me + d) % n
        pltpu.make_async_remote_copy(
            src_ref=x_ref.at[source],
            dst_ref=out_ref.at[source],
            send_sem=send_sem.at[d],
            recv_sem=recv_sem.at[source],
            device_id={"seq": source},
            device_id_type=MESH,
        ).wait_recv()
    for copy in sent:
        copy.wait_send()
    local.wait()


def stats_exchange(n, x):
    dma = pltpu.SemaphoreType.DMA
    return pl.pallas_call(
        functools.partial(stats_kernel, n),
        out_shape=jax.ShapeDtypeStruct(x.shape, x.dtype),
        in_specs=[pl.BlockSpec(memory_space=VMEM)],
        out_specs=pl.BlockSpec(memory_space=VMEM),
        scratch_shapes=[dma((n,)), dma((n,)), dma],
        compiler_params=pltpu.CompilerParams(collective_id=3, has_side_effects=True),
        name="stats",
    )(x)


def per_device(
    n,
    cont_query,
    cont_key,
    cont_value,
    prefix_key,
    prefix_value,
    out_weight,
    norm_gain,
    lm_head,
    target_ids,
    cont_len,
    prompt_len,
    group_of,
    rewards,
):
    cont_count, cont_span, query_width = cont_query.shape
    own_rows = cont_count * cont_span
    planes = cont_key.shape[2] // HD
    lanes = n // planes
    total_rows = own_rows * n
    device_index = lax.axis_index("seq")
    lane = device_index % lanes

    meta = jnp.zeros((8, 128), jnp.float32)
    meta = meta.at[0, :own_rows].set(target_ids.reshape(own_rows).astype(jnp.float32))
    meta = meta.at[1, :cont_count].set(rewards)
    q, ck, cv, pk, pv, meta = exchange(
        n, planes, cont_query, cont_key, cont_value, prefix_key, prefix_value, meta
    )

    def by_lane(x):
        return jnp.swapaxes(x.reshape((planes, lanes) + x.shape[1:]), 0, 1)

    lane_groups = lax.dynamic_index_in_dim(
        by_lane(group_of.reshape(n, cont_count)), lane, 0, keepdims=False
    ).reshape(planes * cont_count)
    attended = attention(lane_groups, prompt_len, q, ck, cv, pk, pv)
    tokens = gather(
        tokens_kernel, n, planes, attended, (total_rows, query_width), 1, "tokens"
    )
    hidden_cols = lax.dot_general(
        out_weight, tokens, (((0,), (1,)), ((), ())), preferred_element_type=jnp.float32
    ).astype(jnp.bfloat16)
    whole = gather(
        features_kernel, n, planes, hidden_cols, (out_weight.shape[0], total_rows), 2, "features"
    )
    widened = whole.astype(jnp.float32)
    factor = lax.rsqrt(jnp.mean(widened * widened, axis=0, keepdims=True) + EPSILON)
    normed = (widened * factor * norm_gain[:, None]).astype(jnp.bfloat16).T

    ids = by_lane(meta[:, 0, :own_rows]).reshape(total_rows, 1).astype(jnp.int32)
    offset = (device_index * lm_head.shape[1]).astype(jnp.int32).reshape(1)
    peak, mass, pick = logit_stats(normed, ids, lm_head, offset)
    top = jnp.max(peak, axis=1)
    mass = jnp.sum(mass * jnp.exp(peak - top[:, None]), axis=1)
    pick = jnp.sum(pick, axis=1)
    stacked = jnp.stack([top, mass, pick]).reshape(3, lanes, planes, own_rows)
    stacked = stacked.transpose(2, 1, 0, 3).reshape(n, 3, own_rows)
    stacked = jnp.pad(stacked, ((0, 0), (0, 5), (0, 128 - own_rows)))
    shares = stats_exchange(n, stacked)[:, :3, :own_rows]
    maximum = jnp.max(shares[:, 0], axis=0)
    total_mass = jnp.sum(shares[:, 1] * jnp.exp(shares[:, 0] - maximum[None, :]), axis=0)
    picked = jnp.sum(shares[:, 2], axis=0)
    logprob = (picked - maximum - jnp.log(total_mass)).reshape(cont_count, cont_span)
    position = jnp.arange(cont_span, dtype=jnp.int32)
    live = position[None, :] < cont_len[:, None]
    token_logprob = jnp.where(live, logprob, 0.0)

    every_reward = meta[:, 1, :cont_count].reshape(n * cont_count)
    own_groups = lax.dynamic_slice_in_dim(group_of, device_index * cont_count, cont_count)
    same = (own_groups[:, None] == group_of[None, :]).astype(jnp.float32)
    group_mean = jnp.sum(same * every_reward[None, :], axis=1) / GROUP
    deviation = every_reward[None, :] - group_mean[:, None]
    spread = jnp.sqrt(jnp.sum(same * deviation * deviation, axis=1) / (GROUP - 1))
    advantage = (rewards - group_mean) / jnp.maximum(spread, REWARD_FLOOR)
    objective = advantage * jnp.sum(token_logprob, axis=1) / cont_len.astype(jnp.float32)
    return (token_logprob, advantage, objective)


def solution(mesh):
    placed = (
        P(("grp", "seq"), None, None),
        P(("grp", "seq"), None, None),
        P(("grp", "seq"), None, None),
        P("grp", "seq", None),
        P("grp", "seq", None),
        P(None, "seq"),
        P(),
        P(None, "seq"),
        P(("grp", "seq"), None),
        P(("grp", "seq")),
        P("grp"),
        P("grp"),
        P(("grp", "seq")),
    )
    return jax.shard_map(
        functools.partial(per_device, mesh.shape["seq"]),
        mesh=mesh,
        in_specs=placed,
        out_specs=(P(("grp", "seq"), None), P(("grp", "seq")), P(("grp", "seq"))),
        check_vma=False,
    )
```

```python
import functools

import jax
import jax.numpy as jnp
from jax import lax
from jax.experimental import pallas as pl
from jax.experimental.pallas import tpu as pltpu
from jax.sharding import PartitionSpec as P

HD = 128
GROUP = 16
NEGATIVE = -1e30
EPSILON = 1e-06
REWARD_FLOOR = 0.25
MESH = pl.DeviceIdType.MESH
VMEM = pltpu.VMEM
LIMIT = 60 * 1024 * 1024


class Place:
    def __init__(self, n, planes):
        self.n, self.planes = n, planes
        self.lanes = n // planes
        self.half = self.lanes // 2
        self.me = lax.axis_index("seq")
        self.plane = self.me // self.lanes
        lane = self.me % self.lanes
        self.row = lane // 2
        self.core = lane % 2

    def device(self, plane, row, core):
        return plane * self.lanes + row * 2 + core

    def plane_at(self, step):
        return (self.plane + step) % self.planes

    def row_at(self, step):
        return (self.row + step) % self.half

    def peers(self):
        out = [self.device(self.plane_at(d), self.row, self.core) for d in range(1, self.planes)]
        out += [self.device(self.plane, self.row_at(e), self.core) for e in range(1, self.half)]
        return out + [self.device(self.plane, self.row, 1 - self.core)]


def greet(peers):
    barrier = pltpu.get_barrier_semaphore()
    for peer in peers:
        pl.semaphore_signal(barrier, inc=1, device_id={"seq": peer}, device_id_type=MESH)
    pl.semaphore_wait(barrier, len(peers))


def send_count(n, planes):
    half = n // planes // 2
    return (planes - 1) + half + (planes - 1) * half + planes * (half - 1)


class Spread:
    def __init__(self, at, parts, own, full, send_sem, recv_sem, local_sem, ring=True):
        self.ring = ring
        self.at, self.parts, self.own, self.full = at, parts, own, full
        self.send_sem, self.recv_sem, self.local_sem = send_sem, recv_sem, local_sem
        self.sent = []

    def send(self, src_ref, source, part, target):
        copy = pltpu.make_async_remote_copy(
            src_ref=src_ref,
            dst_ref=self.full(source, part),
            send_sem=self.send_sem.at[len(self.sent)],
            recv_sem=self.recv_sem.at[source * self.parts + part],
            device_id={"seq": target},
            device_id_type=MESH,
        )
        copy.start()
        self.sent.append(copy)

    def arrived(self, source, part):
        pltpu.make_async_remote_copy(
            src_ref=self.full(source, part),
            dst_ref=self.full(source, part),
            send_sem=self.send_sem.at[0],
            recv_sem=self.recv_sem.at[source * self.parts + part],
            device_id={"seq": self.at.device(self.at.plane, self.at.row, 1 - self.at.core)},
            device_id_type=MESH,
        ).wait_recv()

    def to_rows(self, src_ref, source, part):
        at = self.at
        for e in range(1, at.half):
            self.send(src_ref, source, part, at.device(at.plane, at.row_at(e), at.core))

    def to_core(self, src_ref, source, part):
        at = self.at
        self.send(src_ref, source, part, at.device(at.plane, at.row, 1 - at.core))

    def start(self):
        at = self.at
        self.local = []
        for part in range(self.parts):
            for d in range(1, 2 if self.ring else at.planes):
                target = at.plane_at(d)
                self.send(
                    self.own(part, target), at.me, part, at.device(target, at.row, at.core)
                )
            self.to_rows(self.own(part, at.plane), at.me, part)
            self.to_core(self.own(part, at.plane), at.me, part)
            copy = pltpu.make_async_copy(
                self.own(part, at.plane), self.full(at.me, part), self.local_sem.at[part]
            )
            copy.start()
            self.local.append(copy)

    def from_rows(self, plane):
        at = self.at
        for part in range(self.parts):
            for e in range(1, at.half):
                source = at.device(plane, at.row_at(e), at.core)
                self.arrived(source, part)
                self.to_core(self.full(source, part), source, part)

    def from_plane(self, plane, onward):
        at = self.at
        for part in range(self.parts):
            source = at.device(plane, at.row, at.core)
            self.arrived(source, part)
            if onward:
                target = at.device(at.plane_at(1), at.row, at.core)
                self.send(self.full(source, part), source, part, target)
            self.to_rows(self.full(source, part), source, part)
            self.to_core(self.full(source, part), source, part)

    def finish(self):
        at = self.at
        steps = [1, at.planes - 1] + list(range(2, at.planes - 1))
        if self.ring:
            steps = list(range(at.planes - 1, 0, -1))
        order = [at.plane_at(d) for d in steps]
        self.from_rows(at.plane)
        for i, plane in enumerate(order):
            self.from_plane(plane, self.ring and steps[i] > 1)
            if i >= 1:
                self.from_rows(order[i - 1])
        self.from_rows(order[-1])
        for plane in range(at.planes):
            for row in range(at.half):
                for part in range(self.parts):
                    self.arrived(at.device(plane, row, 1 - at.core), part)
        for copy in self.sent:
            copy.wait_send()
        for copy in self.local:
            copy.wait()


def exchange_kernel(
    n,
    planes,
    q_ref,
    ck_ref,
    cv_ref,
    pk_ref,
    pv_ref,
    meta_ref,
    q_out,
    ck_out,
    cv_out,
    pk_out,
    pv_out,
    meta_out,
    send_sem,
    recv_sem,
    local_sem,
    lane_send,
    lane_recv,
    lane_local,
    meta_send,
    meta_recv,
    meta_local,
):
    at = Place(n, planes)
    greet([(at.me + d) % n for d in range(1, n)])
    conts = q_ref.shape[0]
    span = pk_ref.shape[1]

    def head(ref, plane):
        width = ref.shape[2] // planes
        return ref.at[:, :, pl.ds(pl.multiple_of(plane * width, 128), width)]

    def own(part, plane):
        return head((pk_ref, pv_ref)[part], plane)

    def full(source, part):
        start = pl.multiple_of(source * span, 128)
        return (pk_out, pv_out)[part].at[:, pl.ds(start, span), :]

    spread = Spread(at, 2, own, full, send_sem, recv_sem, local_sem, ring=False)
    spread.start()
    pairs = ((q_ref, q_out), (ck_ref, ck_out), (cv_ref, cv_out))
    waits = []
    for i, (src, dst) in enumerate(pairs):
        mine = dst.at[pl.ds(at.plane * conts, conts)]
        for d in range(1, planes):
            target = at.plane_at(d)
            copy = pltpu.make_async_remote_copy(
                src_ref=head(src, target),
                dst_ref=mine,
                send_sem=lane_send.at[i * planes + d],
                recv_sem=lane_recv.at[i * planes + at.plane],
                device_id={"seq": at.device(target, at.row, at.core)},
                device_id_type=MESH,
            )
            copy.start()
            waits.append(copy.wait_send)
        copy = pltpu.make_async_copy(head(src, at.plane), mine, lane_local.at[i])
        copy.start()
        waits.append(copy.wait)
    for d in range(1, n):
        copy = pltpu.make_async_remote_copy(
            src_ref=meta_ref,
            dst_ref=meta_out.at[at.me],
            send_sem=meta_send.at[d],
            recv_sem=meta_recv.at[at.me],
            device_id={"seq": (at.me + d) % n},
            device_id_type=MESH,
        )
        copy.start()
        waits.append(copy.wait_send)
    copy = pltpu.make_async_copy(meta_ref, meta_out.at[at.me], meta_local)
    copy.start()
    waits.append(copy.wait)
    spread.finish()
    for i, (src, dst) in enumerate(pairs):
        for d in range(1, planes):
            source = at.plane_at(d)
            landed = dst.at[pl.ds(source * conts, conts)]
            pltpu.make_async_remote_copy(
                src_ref=landed,
                dst_ref=landed,
                send_sem=lane_send.at[i * planes + d],
                recv_sem=lane_recv.at[i * planes + source],
                device_id={"seq": at.device(source, at.row, at.core)},
                device_id_type=MESH,
            ).wait_recv()
    for d in range(1, n):
        source = (at.me + d) % n
        pltpu.make_async_remote_copy(
            src_ref=meta_ref,
            dst_ref=meta_out.at[source],
            send_sem=meta_send.at[d],
            recv_sem=meta_recv.at[source],
            device_id={"seq": source},
            device_id_type=MESH,
        ).wait_recv()
    for wait in waits:
        wait()


def exchange(n, planes, q, ck, cv, pk, pv, meta):
    conts, steps, width = q.shape
    prompts, span, _ = pk.shape
    dma = pltpu.SemaphoreType.DMA
    shape = jax.ShapeDtypeStruct
    return pl.pallas_call(
        functools.partial(exchange_kernel, n, planes),
        out_shape=(
            shape((conts * planes, steps, width // planes), q.dtype),
            shape((conts * planes, steps, ck.shape[2] // planes), q.dtype),
            shape((conts * planes, steps, ck.shape[2] // planes), q.dtype),
            shape((prompts, span * n, pk.shape[2] // planes), q.dtype),
            shape((prompts, span * n, pk.shape[2] // planes), q.dtype),
            shape((n,) + meta.shape, meta.dtype),
        ),
        in_specs=[pl.BlockSpec(memory_space=VMEM)] * 6,
        out_specs=(pl.BlockSpec(memory_space=VMEM),) * 6,
        scratch_shapes=[
            dma((2 * send_count(n, planes),)),
            dma((2 * n,)),
            dma((2,)),
            dma((3 * planes,)),
            dma((3 * planes,)),
            dma((3,)),
            dma((n,)),
            dma((n,)),
            dma,
        ],
        compiler_params=pltpu.CompilerParams(
            collective_id=0, has_side_effects=True, vmem_limit_bytes=LIMIT
        ),
        name="exchange",
    )(q, ck, cv, pk, pv, meta)


def attention_kernel(group_ref, length_ref, q_ref, ck_ref, cv_ref, pk_ref, pv_ref, out_ref):
    cont = pl.program_id(0)
    prompt = group_ref[cont]
    length = length_ref[prompt]
    steps, width = q_ref.shape[1:]
    heads = width // HD
    q = q_ref[0]
    rows = jnp.concatenate([q[:, h * HD : (h + 1) * HD] for h in range(heads)], axis=0)
    contract = (((1,), (1,)), ((), ()))
    early = lax.dot_general(rows, pk_ref[prompt], contract, preferred_element_type=jnp.float32)
    late = lax.dot_general(rows, ck_ref[0], contract, preferred_element_type=jnp.float32)
    scale = HD ** (-0.5)
    column = lax.broadcasted_iota(jnp.int32, early.shape, 1)
    early = jnp.where(column < length, early * scale, NEGATIVE)
    line = lax.broadcasted_iota(jnp.int32, late.shape, 0) % steps
    late = jnp.where(
        lax.broadcasted_iota(jnp.int32, late.shape, 1) <= line, late * scale, NEGATIVE
    )
    peak = jnp.maximum(
        jnp.max(early, axis=1, keepdims=True), jnp.max(late, axis=1, keepdims=True)
    )
    early = jnp.exp(early - peak).astype(jnp.bfloat16)
    late = jnp.exp(late - peak).astype(jnp.bfloat16)
    total = jnp.sum(early.astype(jnp.float32), axis=1, keepdims=True) + jnp.sum(
        late.astype(jnp.float32), axis=1, keepdims=True
    )
    mixed = jnp.dot(early, pv_ref[prompt], preferred_element_type=jnp.float32) + jnp.dot(
        late, cv_ref[0], preferred_element_type=jnp.float32
    )
    mixed = (mixed / total).astype(jnp.bfloat16)
    out_ref[...] = jnp.concatenate(
        [mixed[h * steps : (h + 1) * steps] for h in range(heads)], axis=1
    )


def attention(groups, lengths, q, ck, cv, pk, pv):
    conts, steps, width = q.shape
    whole = pl.BlockSpec(memory_space=VMEM)
    scalar = pl.BlockSpec(memory_space=pltpu.SMEM)
    return pl.pallas_call(
        attention_kernel,
        out_shape=jax.ShapeDtypeStruct((conts * steps, width), jnp.bfloat16),
        grid=(conts,),
        in_specs=[
            scalar,
            scalar,
            pl.BlockSpec((1, steps, width), lambda c: (c, 0, 0)),
            pl.BlockSpec((1, steps, ck.shape[2]), lambda c: (c, 0, 0)),
            pl.BlockSpec((1, steps, ck.shape[2]), lambda c: (c, 0, 0)),
            whole,
            whole,
        ],
        out_specs=pl.BlockSpec((steps, width), lambda c: (c, 0)),
        compiler_params=pltpu.CompilerParams(vmem_limit_bytes=LIMIT),
        name="attention",
    )(groups, lengths, q, ck, cv, pk, pv)


PARTS = 2


def tokens_kernel(n, planes, x_ref, out_ref, send_sem, recv_sem, local_sem):
    at = Place(n, planes)
    greet(at.peers())
    rows, width = x_ref.shape
    piece = rows // PARTS

    def own(part, plane):
        return x_ref.at[pl.ds(part * piece, piece)]

    def full(source, part):
        start = pl.multiple_of(source % at.lanes * rows + part * piece, 16)
        column = pl.multiple_of(source // at.lanes * width, 128)
        return out_ref.at[pl.ds(start, piece), pl.ds(column, width)]

    spread = Spread(at, PARTS, own, full, send_sem, recv_sem, local_sem)
    spread.start()
    spread.finish()


def features_kernel(n, planes, x_ref, out_ref, send_sem, recv_sem, local_sem):
    at = Place(n, planes)
    greet(at.peers())
    rows, width = x_ref.shape
    piece = width // PARTS

    def own(part, plane):
        return x_ref.at[:, pl.ds(part * piece, piece)]

    def full(source, part):
        start = pl.multiple_of(source * rows, 16)
        return out_ref.at[pl.ds(start, rows), pl.ds(part * piece, piece)]

    spread = Spread(at, PARTS, own, full, send_sem, recv_sem, local_sem)
    spread.start()
    spread.finish()


def gather(kernel, n, planes, x, shape, number, name):
    dma = pltpu.SemaphoreType.DMA
    return pl.pallas_call(
        functools.partial(kernel, n, planes),
        out_shape=jax.ShapeDtypeStruct(shape, x.dtype),
        in_specs=[pl.BlockSpec(memory_space=VMEM)],
        out_specs=pl.BlockSpec(memory_space=VMEM),
        scratch_shapes=[
            dma((PARTS * send_count(n, planes),)),
            dma((PARTS * n,)),
            dma((PARTS,)),
        ],
        compiler_params=pltpu.CompilerParams(
            collective_id=number, has_side_effects=True, vmem_limit_bytes=LIMIT
        ),
        name=name,
    )(x)


TILE = 528
BAND = 512
STEP = 128


def logits_kernel(
    vocab, offset_ref, x_ref, gain_ref, ids_ref, head_ref, max_ref, sum_ref, pick_ref, normed_ref
):
    step = pl.program_id(0)
    depth, tokens = x_ref.shape

    @pl.when(step == 0)
    def _():
        max_ref[...] = jnp.full_like(max_ref, NEGATIVE)
        sum_ref[...] = jnp.zeros_like(sum_ref)
        pick_ref[...] = jnp.zeros_like(pick_ref)

        def square(i, total):
            rows = x_ref[pl.ds(pl.multiple_of(i * STEP, STEP), STEP)].astype(jnp.float32)
            return total + jnp.sum((rows * rows).reshape(STEP // 8, 8, tokens), axis=0)

        total = lax.fori_loop(0, depth // STEP, square, jnp.zeros((8, tokens), jnp.float32))
        mean = jnp.sum(total, axis=0, keepdims=True) / depth
        factor = lax.rsqrt(mean + EPSILON)

        @pl.loop(0, depth // STEP)
        def _(i):
            at = pl.ds(pl.multiple_of(i * STEP, STEP), STEP)
            rows = x_ref[at].astype(jnp.float32)
            normed_ref[at] = (rows * factor * gain_ref[at]).astype(jnp.bfloat16)

    head = head_ref[...]
    base = step * TILE
    for start in range(0, tokens, BAND):
        band = slice(start, start + BAND)
        logits = jnp.dot(head, normed_ref[:, band], preferred_element_type=jnp.float32)
        row = base + lax.broadcasted_iota(jnp.int32, logits.shape, 0)
        wanted = ids_ref[:, band] - offset_ref[0]
        if vocab % TILE:
            wanted = jnp.where(wanted < vocab, wanted, -1)
            logits = jnp.where(row < vocab, logits, NEGATIVE)
        chosen = jnp.where(row == wanted, logits, 0.0)
        split = (TILE // 8, 8, BAND)
        before = max_ref[:, band]
        best = jnp.maximum(before, jnp.max(logits.reshape(split), axis=0))
        mass = jnp.sum(jnp.exp(logits.reshape(split) - best[None]), axis=0)
        max_ref[:, band] = best
        sum_ref[:, band] = sum_ref[:, band] * jnp.exp(before - best) + mass
        pick_ref[:, band] += jnp.sum(chosen.reshape(split), axis=0)


def logit_stats(x, gain, ids, head, offset):
    depth, tokens = x.shape
    vocab = head.shape[0]
    whole = pl.BlockSpec((8, tokens), lambda v: (0, 0))
    return pl.pallas_call(
        functools.partial(logits_kernel, vocab),
        out_shape=(jax.ShapeDtypeStruct((8, tokens), jnp.float32),) * 3,
        grid=(pl.cdiv(vocab, TILE),),
        in_specs=[
            pl.BlockSpec(memory_space=pltpu.SMEM),
            pl.BlockSpec(memory_space=VMEM),
            pl.BlockSpec(memory_space=VMEM),
            pl.BlockSpec(memory_space=VMEM),
            pl.BlockSpec((TILE, depth), lambda v: (v, 0)),
        ],
        out_specs=(whole,) * 3,
        scratch_shapes=[VMEM((depth, tokens), jnp.bfloat16)],
        compiler_params=pltpu.CompilerParams(vmem_limit_bytes=LIMIT),
        name="logits",
    )(offset, x, gain, ids, head)


def stats_kernel(n, x_ref, out_ref, send_sem, recv_sem, local_sem):
    me = lax.axis_index("seq")
    greet([(me + d) % n for d in range(1, n)])
    sent = []
    for d in range(1, n):
        target = (me + d) % n
        copy = pltpu.make_async_remote_copy(
            src_ref=x_ref.at[target],
            dst_ref=out_ref.at[me],
            send_sem=send_sem.at[d],
            recv_sem=recv_sem.at[me],
            device_id={"seq": target},
            device_id_type=MESH,
        )
        copy.start()
        sent.append(copy)
    local = pltpu.make_async_copy(x_ref.at[me], out_ref.at[me], local_sem)
    local.start()
    for d in range(1, n):
        source = (me + d) % n
        pltpu.make_async_remote_copy(
            src_ref=x_ref.at[source],
            dst_ref=out_ref.at[source],
            send_sem=send_sem.at[d],
            recv_sem=recv_sem.at[source],
            device_id={"seq": source},
            device_id_type=MESH,
        ).wait_recv()
    for copy in sent:
        copy.wait_send()
    local.wait()


def stats_exchange(n, x):
    dma = pltpu.SemaphoreType.DMA
    return pl.pallas_call(
        functools.partial(stats_kernel, n),
        out_shape=jax.ShapeDtypeStruct(x.shape, x.dtype),
        in_specs=[pl.BlockSpec(memory_space=VMEM)],
        out_specs=pl.BlockSpec(memory_space=VMEM),
        scratch_shapes=[dma((n,)), dma((n,)), dma],
        compiler_params=pltpu.CompilerParams(collective_id=3, has_side_effects=True),
        name="stats",
    )(x)


def per_device(
    n,
    cont_query,
    cont_key,
    cont_value,
    prefix_key,
    prefix_value,
    out_weight,
    norm_gain,
    lm_head,
    target_ids,
    cont_len,
    prompt_len,
    group_of,
    rewards,
):
    cont_count, cont_span, query_width = cont_query.shape
    own_rows = cont_count * cont_span
    planes = cont_key.shape[2] // HD
    lanes = n // planes
    total_rows = own_rows * n
    device_index = lax.axis_index("seq")
    lane = device_index % lanes

    meta = jnp.zeros((8, 128), jnp.float32)
    meta = meta.at[0, :own_rows].set(target_ids.reshape(own_rows).astype(jnp.float32))
    meta = meta.at[1, :cont_count].set(rewards)
    q, ck, cv, pk, pv, meta = exchange(
        n, planes, cont_query, cont_key, cont_value, prefix_key, prefix_value, meta
    )

    def by_lane(x):
        return jnp.swapaxes(x.reshape((planes, lanes) + x.shape[1:]), 0, 1)

    lane_groups = lax.dynamic_index_in_dim(
        by_lane(group_of.reshape(n, cont_count)), lane, 0, keepdims=False
    ).reshape(planes * cont_count)
    attended = attention(lane_groups, prompt_len, q, ck, cv, pk, pv)
    tokens = gather(
        tokens_kernel, n, planes, attended, (total_rows, query_width), 1, "tokens"
    )
    hidden_cols = lax.dot_general(
        out_weight, tokens, (((0,), (1,)), ((), ())), preferred_element_type=jnp.float32
    ).astype(jnp.bfloat16)
    whole = gather(
        features_kernel, n, planes, hidden_cols, (out_weight.shape[0], total_rows), 2, "features"
    )
    ids = by_lane(meta[:, 0, :own_rows]).reshape(1, total_rows).astype(jnp.int32)
    offset = (device_index * lm_head.shape[1]).astype(jnp.int32).reshape(1)
    peak, mass, pick = logit_stats(whole, norm_gain[:, None], ids, lm_head.T, offset)
    top = jnp.max(peak, axis=0)
    mass = jnp.sum(mass * jnp.exp(peak - top[None, :]), axis=0)
    pick = jnp.sum(pick, axis=0)
    stacked = jnp.stack([top, mass, pick]).reshape(3, lanes, planes, own_rows)
    stacked = stacked.transpose(2, 1, 0, 3).reshape(n, 3, own_rows)
    stacked = jnp.pad(stacked, ((0, 0), (0, 5), (0, 128 - own_rows)))
    shares = stats_exchange(n, stacked)[:, :3, :own_rows]
    maximum = jnp.max(shares[:, 0], axis=0)
    total_mass = jnp.sum(shares[:, 1] * jnp.exp(shares[:, 0] - maximum[None, :]), axis=0)
    picked = jnp.sum(shares[:, 2], axis=0)
    logprob = (picked - maximum - jnp.log(total_mass)).reshape(cont_count, cont_span)
    position = jnp.arange(cont_span, dtype=jnp.int32)
    live = position[None, :] < cont_len[:, None]
    token_logprob = jnp.where(live, logprob, 0.0)

    every_reward = meta[:, 1, :cont_count].reshape(n * cont_count)
    own_groups = lax.dynamic_slice_in_dim(group_of, device_index * cont_count, cont_count)
    same = (own_groups[:, None] == group_of[None, :]).astype(jnp.float32)
    group_mean = jnp.sum(same * every_reward[None, :], axis=1) / GROUP
    deviation = every_reward[None, :] - group_mean[:, None]
    spread = jnp.sqrt(jnp.sum(same * deviation * deviation, axis=1) / (GROUP - 1))
    advantage = (rewards - group_mean) / jnp.maximum(spread, REWARD_FLOOR)
    objective = advantage * jnp.sum(token_logprob, axis=1) / cont_len.astype(jnp.float32)
    return (token_logprob, advantage, objective)


def solution(mesh):
    placed = (
        P(("grp", "seq"), None, None),
        P(("grp", "seq"), None, None),
        P(("grp", "seq"), None, None),
        P("grp", "seq", None),
        P("grp", "seq", None),
        P(None, "seq"),
        P(),
        P(None, "seq"),
        P(("grp", "seq"), None),
        P(("grp", "seq")),
        P("grp"),
        P("grp"),
        P(("grp", "seq")),
    )
    return jax.shard_map(
        functools.partial(per_device, mesh.shape["seq"]),
        mesh=mesh,
        in_specs=placed,
        out_specs=(P(("grp", "seq"), None), P(("grp", "seq")), P(("grp", "seq"))),
        check_vma=False,
    )
```

```python
import functools

import jax
import jax.numpy as jnp
from jax import lax
from jax.experimental import pallas as pl
from jax.experimental.pallas import tpu as pltpu
from jax.sharding import PartitionSpec as P

HD = 128
GROUP = 16
NEGATIVE = -1e30
EPSILON = 1e-06
REWARD_FLOOR = 0.25
MESH = pl.DeviceIdType.MESH
VMEM = pltpu.VMEM
LIMIT = 60 * 1024 * 1024


class Place:
    def __init__(self, n, planes):
        self.n, self.planes = n, planes
        self.lanes = n // planes
        self.half = self.lanes // 2
        self.me = lax.axis_index("seq")
        self.plane = self.me // self.lanes
        lane = self.me % self.lanes
        self.row = lane // 2
        self.core = lane % 2

    def device(self, plane, row, core):
        return plane * self.lanes + row * 2 + core

    def plane_at(self, step):
        return (self.plane + step) % self.planes

    def row_at(self, step):
        return (self.row + step) % self.half

    def peers(self):
        out = [self.device(self.plane_at(d), self.row, self.core) for d in range(1, self.planes)]
        out += [self.device(self.plane, self.row_at(e), self.core) for e in range(1, self.half)]
        return out + [self.device(self.plane, self.row, 1 - self.core)]


def greet(peers):
    barrier = pltpu.get_barrier_semaphore()
    for peer in peers:
        pl.semaphore_signal(barrier, inc=1, device_id={"seq": peer}, device_id_type=MESH)
    pl.semaphore_wait(barrier, len(peers))


def send_count(n, planes):
    half = n // planes // 2
    return (planes - 1) + half + (planes - 1) * half + planes * (half - 1)


class Spread:
    def __init__(self, at, parts, own, full, send_sem, recv_sem, local_sem, ring=True):
        self.ring = ring
        self.at, self.parts, self.own, self.full = at, parts, own, full
        self.send_sem, self.recv_sem, self.local_sem = send_sem, recv_sem, local_sem
        self.sent = []

    def send(self, src_ref, source, part, target):
        copy = pltpu.make_async_remote_copy(
            src_ref=src_ref,
            dst_ref=self.full(source, part),
            send_sem=self.send_sem.at[len(self.sent)],
            recv_sem=self.recv_sem.at[source * self.parts + part],
            device_id={"seq": target},
            device_id_type=MESH,
        )
        copy.start()
        self.sent.append(part)

    def arrived(self, source, part):
        pltpu.make_async_remote_copy(
            src_ref=self.full(source, part),
            dst_ref=self.full(source, part),
            send_sem=self.send_sem.at[0],
            recv_sem=self.recv_sem.at[source * self.parts + part],
            device_id={"seq": self.at.device(self.at.plane, self.at.row, 1 - self.at.core)},
            device_id_type=MESH,
        ).wait_recv()

    def to_rows(self, src_ref, source, part):
        at = self.at
        for e in range(1, at.half):
            self.send(src_ref, source, part, at.device(at.plane, at.row_at(e), at.core))

    def to_core(self, src_ref, source, part):
        at = self.at
        self.send(src_ref, source, part, at.device(at.plane, at.row, 1 - at.core))

    def start(self):
        at = self.at
        self.local = []
        for part in range(self.parts):
            for d in range(1, 2 if self.ring else at.planes):
                target = at.plane_at(d)
                self.send(
                    self.own(part, target), at.me, part, at.device(target, at.row, at.core)
                )
            self.to_rows(self.own(part, at.plane), at.me, part)
            self.to_core(self.own(part, at.plane), at.me, part)
            copy = pltpu.make_async_copy(
                self.own(part, at.plane), self.full(at.me, part), self.local_sem.at[part]
            )
            copy.start()
            self.local.append(copy)

    def from_rows(self, plane, part):
        at = self.at
        for e in range(1, at.half):
            source = at.device(plane, at.row_at(e), at.core)
            self.arrived(source, part)
            self.to_core(self.full(source, part), source, part)

    def from_plane(self, step, part):
        at = self.at
        source = at.device(at.plane_at(step), at.row, at.core)
        self.arrived(source, part)
        if self.ring and step > 1:
            target = at.device(at.plane_at(1), at.row, at.core)
            self.send(self.full(source, part), source, part, target)
        self.to_rows(self.full(source, part), source, part)
        self.to_core(self.full(source, part), source, part)

    def events(self, part):
        at = self.at
        steps = [1, at.planes - 1] + list(range(2, at.planes - 1))
        if self.ring:
            steps = list(range(at.planes - 1, 0, -1))
        listed = [functools.partial(self.from_rows, at.plane, part)]
        for i, step in enumerate(steps):
            listed.append(functools.partial(self.from_plane, step, part))
            if i >= 1:
                listed.append(functools.partial(self.from_rows, at.plane_at(steps[i - 1]), part))
        listed.append(functools.partial(self.from_rows, at.plane_at(steps[-1]), part))
        return listed

    def from_core(self, part):
        at = self.at
        for plane in range(at.planes):
            for row in range(at.half):
                self.arrived(at.device(plane, row, 1 - at.core), part)

    def drain(self):
        at = self.at
        for i, part in enumerate(self.sent):
            pltpu.make_async_remote_copy(
                src_ref=self.full(at.me, part),
                dst_ref=self.full(at.me, part),
                send_sem=self.send_sem.at[i],
                recv_sem=self.recv_sem.at[0],
                device_id={"seq": at.device(at.plane, at.row, 1 - at.core)},
                device_id_type=MESH,
            ).wait_send()

    def finish(self):
        for both in zip(*[self.events(part) for part in range(self.parts)]):
            for event in both:
                event()
        for part in range(self.parts):
            self.from_core(part)
        self.drain()
        for copy in self.local:
            copy.wait()


def exchange_kernel(
    n,
    planes,
    q_ref,
    ck_ref,
    cv_ref,
    pk_ref,
    pv_ref,
    meta_ref,
    q_out,
    ck_out,
    cv_out,
    pk_out,
    pv_out,
    meta_out,
    send_sem,
    recv_sem,
    local_sem,
    lane_send,
    lane_recv,
    lane_local,
    meta_send,
    meta_recv,
    meta_local,
):
    at = Place(n, planes)
    greet([(at.me + d) % n for d in range(1, n)])
    conts = q_ref.shape[0]
    span = pk_ref.shape[1]

    def head(ref, plane):
        width = ref.shape[2] // planes
        return ref.at[:, :, pl.ds(pl.multiple_of(plane * width, 128), width)]

    def own(part, plane):
        return head((pk_ref, pv_ref)[part], plane)

    def full(source, part):
        start = pl.multiple_of(source * span, 128)
        return (pk_out, pv_out)[part].at[:, pl.ds(start, span), :]

    spread = Spread(at, 2, own, full, send_sem, recv_sem, local_sem, ring=False)
    spread.start()
    pairs = ((q_ref, q_out), (ck_ref, ck_out), (cv_ref, cv_out))
    waits = []
    for i, (src, dst) in enumerate(pairs):
        mine = dst.at[pl.ds(at.plane * conts, conts)]
        for d in range(1, planes):
            target = at.plane_at(d)
            copy = pltpu.make_async_remote_copy(
                src_ref=head(src, target),
                dst_ref=mine,
                send_sem=lane_send.at[i * planes + d],
                recv_sem=lane_recv.at[i * planes + at.plane],
                device_id={"seq": at.device(target, at.row, at.core)},
                device_id_type=MESH,
            )
            copy.start()
            waits.append(copy.wait_send)
        copy = pltpu.make_async_copy(head(src, at.plane), mine, lane_local.at[i])
        copy.start()
        waits.append(copy.wait)
    for d in range(1, n):
        copy = pltpu.make_async_remote_copy(
            src_ref=meta_ref,
            dst_ref=meta_out.at[at.me],
            send_sem=meta_send.at[d],
            recv_sem=meta_recv.at[at.me],
            device_id={"seq": (at.me + d) % n},
            device_id_type=MESH,
        )
        copy.start()
        waits.append(copy.wait_send)
    copy = pltpu.make_async_copy(meta_ref, meta_out.at[at.me], meta_local)
    copy.start()
    waits.append(copy.wait)
    spread.finish()
    for i, (src, dst) in enumerate(pairs):
        for d in range(1, planes):
            source = at.plane_at(d)
            landed = dst.at[pl.ds(source * conts, conts)]
            pltpu.make_async_remote_copy(
                src_ref=landed,
                dst_ref=landed,
                send_sem=lane_send.at[i * planes + d],
                recv_sem=lane_recv.at[i * planes + source],
                device_id={"seq": at.device(source, at.row, at.core)},
                device_id_type=MESH,
            ).wait_recv()
    for d in range(1, n):
        source = (at.me + d) % n
        pltpu.make_async_remote_copy(
            src_ref=meta_ref,
            dst_ref=meta_out.at[source],
            send_sem=meta_send.at[d],
            recv_sem=meta_recv.at[source],
            device_id={"seq": source},
            device_id_type=MESH,
        ).wait_recv()
    for wait in waits:
        wait()


def exchange(n, planes, q, ck, cv, pk, pv, meta):
    conts, steps, width = q.shape
    prompts, span, _ = pk.shape
    dma = pltpu.SemaphoreType.DMA
    shape = jax.ShapeDtypeStruct
    return pl.pallas_call(
        functools.partial(exchange_kernel, n, planes),
        out_shape=(
            shape((conts * planes, steps, width // planes), q.dtype),
            shape((conts * planes, steps, ck.shape[2] // planes), q.dtype),
            shape((conts * planes, steps, ck.shape[2] // planes), q.dtype),
            shape((prompts, span * n, pk.shape[2] // planes), q.dtype),
            shape((prompts, span * n, pk.shape[2] // planes), q.dtype),
            shape((n,) + meta.shape, meta.dtype),
        ),
        in_specs=[pl.BlockSpec(memory_space=VMEM)] * 6,
        out_specs=(pl.BlockSpec(memory_space=VMEM),) * 6,
        scratch_shapes=[
            dma((2 * send_count(n, planes),)),
            dma((2 * n,)),
            dma((2,)),
            dma((3 * planes,)),
            dma((3 * planes,)),
            dma((3,)),
            dma((n,)),
            dma((n,)),
            dma,
        ],
        compiler_params=pltpu.CompilerParams(
            collective_id=0, has_side_effects=True, vmem_limit_bytes=LIMIT
        ),
        name="exchange",
    )(q, ck, cv, pk, pv, meta)


def attention_kernel(group_ref, length_ref, q_ref, ck_ref, cv_ref, pk_ref, pv_ref, out_ref):
    cont = pl.program_id(0)
    prompt = group_ref[cont]
    length = length_ref[prompt]
    steps, width = q_ref.shape[1:]
    heads = width // HD
    q = q_ref[0]
    rows = jnp.concatenate([q[:, h * HD : (h + 1) * HD] for h in range(heads)], axis=0)
    contract = (((1,), (1,)), ((), ()))
    early = lax.dot_general(rows, pk_ref[prompt], contract, preferred_element_type=jnp.float32)
    late = lax.dot_general(rows, ck_ref[0], contract, preferred_element_type=jnp.float32)
    scale = HD ** (-0.5)
    column = lax.broadcasted_iota(jnp.int32, early.shape, 1)
    early = jnp.where(column < length, early * scale, NEGATIVE)
    line = lax.broadcasted_iota(jnp.int32, late.shape, 0) % steps
    late = jnp.where(
        lax.broadcasted_iota(jnp.int32, late.shape, 1) <= line, late * scale, NEGATIVE
    )
    peak = jnp.maximum(
        jnp.max(early, axis=1, keepdims=True), jnp.max(late, axis=1, keepdims=True)
    )
    early = jnp.exp(early - peak).astype(jnp.bfloat16)
    late = jnp.exp(late - peak).astype(jnp.bfloat16)
    total = jnp.sum(early.astype(jnp.float32), axis=1, keepdims=True) + jnp.sum(
        late.astype(jnp.float32), axis=1, keepdims=True
    )
    mixed = jnp.dot(early, pv_ref[prompt], preferred_element_type=jnp.float32) + jnp.dot(
        late, cv_ref[0], preferred_element_type=jnp.float32
    )
    mixed = (mixed / total).astype(jnp.bfloat16)
    out_ref[...] = jnp.concatenate(
        [mixed[h * steps : (h + 1) * steps] for h in range(heads)], axis=1
    )


def attention(groups, lengths, q, ck, cv, pk, pv):
    conts, steps, width = q.shape
    whole = pl.BlockSpec(memory_space=VMEM)
    scalar = pl.BlockSpec(memory_space=pltpu.SMEM)
    return pl.pallas_call(
        attention_kernel,
        out_shape=jax.ShapeDtypeStruct((conts * steps, width), jnp.bfloat16),
        grid=(conts,),
        in_specs=[
            scalar,
            scalar,
            pl.BlockSpec((1, steps, width), lambda c: (c, 0, 0)),
            pl.BlockSpec((1, steps, ck.shape[2]), lambda c: (c, 0, 0)),
            pl.BlockSpec((1, steps, ck.shape[2]), lambda c: (c, 0, 0)),
            whole,
            whole,
        ],
        out_specs=pl.BlockSpec((steps, width), lambda c: (c, 0)),
        compiler_params=pltpu.CompilerParams(vmem_limit_bytes=LIMIT),
        name="attention",
    )(groups, lengths, q, ck, cv, pk, pv)


PARTS = 2


def tokens_kernel(n, planes, x_ref, out_ref, send_sem, recv_sem, local_sem):
    at = Place(n, planes)
    greet(at.peers())
    rows, width = x_ref.shape
    piece = rows // PARTS

    def own(part, plane):
        return x_ref.at[pl.ds(part * piece, piece)]

    def full(source, part):
        start = pl.multiple_of(source % at.lanes * rows + part * piece, 16)
        column = pl.multiple_of(source // at.lanes * width, 128)
        return out_ref.at[pl.ds(start, piece), pl.ds(column, width)]

    spread = Spread(at, PARTS, own, full, send_sem, recv_sem, local_sem)
    spread.start()
    spread.finish()


def gather(kernel, n, planes, x, shape, number, name):
    dma = pltpu.SemaphoreType.DMA
    return pl.pallas_call(
        functools.partial(kernel, n, planes),
        out_shape=jax.ShapeDtypeStruct(shape, x.dtype),
        in_specs=[pl.BlockSpec(memory_space=VMEM)],
        out_specs=pl.BlockSpec(memory_space=VMEM),
        scratch_shapes=[
            dma((PARTS * send_count(n, planes),)),
            dma((PARTS * n,)),
            dma((PARTS,)),
        ],
        compiler_params=pltpu.CompilerParams(
            collective_id=number, has_side_effects=True, vmem_limit_bytes=LIMIT
        ),
        name=name,
    )(x)


TILE = 528
BAND = 256
STEP = 128


def scores_kernel(
    n,
    planes,
    offset_ref,
    x_ref,
    gain_ref,
    ids_ref,
    head_hbm,
    out_ref,
    hidden_ref,
    normed_ref,
    head_ref,
    max_ref,
    sum_ref,
    pick_ref,
    send_sem,
    recv_sem,
    local_sem,
    head_sem,
):
    at = Place(n, planes)
    greet(at.peers())
    rows, tokens = x_ref.shape
    depth = rows * n
    vocab = head_hbm.shape[0]
    piece = tokens // PARTS
    tiles, rest = vocab // TILE, vocab % TILE

    def own(part, plane):
        return x_ref.at[:, pl.ds(part * piece, piece)]

    def full(source, part):
        start = pl.multiple_of(source * rows, 16)
        return hidden_ref.at[pl.ds(start, rows), pl.ds(part * piece, piece)]

    spread = Spread(at, PARTS, own, full, send_sem, recv_sem, local_sem)
    spread.start()

    def load(tile, size):
        cut = pl.ds(pl.multiple_of(tile * TILE, 8), size)
        return pltpu.make_async_copy(head_hbm.at[cut], head_ref.at[cut], head_sem.at[tile])

    for tile in range(tiles):
        load(tile, TILE).start()
    if rest:
        load(tiles, rest).start()

    max_ref[...] = jnp.full_like(max_ref, NEGATIVE)
    sum_ref[...] = jnp.zeros_like(sum_ref)
    pick_ref[...] = jnp.zeros_like(pick_ref)

    def normalize(part):
        columns = pl.ds(part * piece, piece)

        def square(i, total):
            cut = pl.ds(pl.multiple_of(i * STEP, STEP), STEP)
            wide = hidden_ref[cut, columns].astype(jnp.float32)
            return total + jnp.sum((wide * wide).reshape(STEP // 8, 8, piece), axis=0)

        total = lax.fori_loop(0, depth // STEP, square, jnp.zeros((8, piece), jnp.float32))
        factor = lax.rsqrt(jnp.sum(total, axis=0, keepdims=True) / depth + EPSILON)

        @pl.loop(0, depth // STEP)
        def _(i):
            cut = pl.ds(pl.multiple_of(i * STEP, STEP), STEP)
            wide = hidden_ref[cut, columns].astype(jnp.float32)
            normed_ref[cut] = (wide * factor * gain_ref[cut]).astype(jnp.bfloat16)

    def score(part, tile, size):
        if part == 0:
            load(tile, size).wait()
        head = head_ref[pl.ds(pl.multiple_of(tile * TILE, 8), size)]
        base = tile * TILE + offset_ref[0]
        products = [
            jnp.dot(head, normed_ref[:, start : start + BAND], preferred_element_type=jnp.float32)
            for start in range(0, piece, BAND)
        ]
        for i, logits in enumerate(products):
            band = slice(part * piece + i * BAND, part * piece + (i + 1) * BAND)
            row = lax.broadcasted_iota(jnp.int32, logits.shape, 0)
            chosen = jnp.where(row == ids_ref[:, band] - base, logits, 0.0)
            split = (size // 8, 8, BAND)
            before = max_ref[:, band]
            best = jnp.maximum(before, jnp.max(logits.reshape(split), axis=0))
            mass = jnp.sum(jnp.exp(logits.reshape(split) - best[None]), axis=0)
            max_ref[:, band] = best
            sum_ref[:, band] = sum_ref[:, band] * jnp.exp(before - best) + mass
            pick_ref[:, band] += jnp.sum(chosen.reshape(split), axis=0)

    def score_all(part, events):
        @pl.loop(0, tiles)
        def _(tile):
            for i, event in enumerate(events):
                pl.when(tile == min(i, tiles - 1))(event)
            score(part, tile, TILE)

        if rest:
            score(part, tiles, rest)

    first, second = spread.events(0), spread.events(1)
    cut = len(first) - 2
    for event in first[:cut] + second[:2] + first[cut:]:
        event()
    spread.from_core(0)
    second[2]()
    spread.local[0].wait()
    normalize(0)
    score_all(0, second[3:])
    spread.from_core(1)
    spread.local[1].wait()
    normalize(1)
    score_all(1, [])
    spread.drain()
    peak = max_ref[...]
    top = jnp.max(peak, axis=0, keepdims=True)
    out_ref[...] = jnp.zeros_like(out_ref)
    out_ref[0:1] = top
    out_ref[1:2] = jnp.sum(sum_ref[...] * jnp.exp(peak - top), axis=0, keepdims=True)
    out_ref[2:3] = jnp.sum(pick_ref[...], axis=0, keepdims=True)


def scores(n, planes, x, gain, ids, head, offset):
    rows, tokens = x.shape
    depth = rows * n
    dma = pltpu.SemaphoreType.DMA
    vmem = pl.BlockSpec(memory_space=VMEM)
    running = VMEM((8, tokens), jnp.float32)
    return pl.pallas_call(
        functools.partial(scores_kernel, n, planes),
        out_shape=jax.ShapeDtypeStruct((8, tokens), jnp.float32),
        in_specs=[
            pl.BlockSpec(memory_space=pltpu.SMEM),
            vmem,
            vmem,
            vmem,
            pl.BlockSpec(memory_space=pl.ANY),
        ],
        out_specs=vmem,
        scratch_shapes=[
            VMEM((depth, tokens), x.dtype),
            VMEM((depth, tokens // PARTS), x.dtype),
            VMEM(head.shape, head.dtype),
            running,
            running,
            running,
            dma((PARTS * send_count(n, planes),)),
            dma((PARTS * n,)),
            dma((PARTS,)),
            dma((pl.cdiv(head.shape[0], TILE),)),
        ],
        compiler_params=pltpu.CompilerParams(
            collective_id=2, has_side_effects=True, vmem_limit_bytes=LIMIT
        ),
        name="scores",
    )(offset, x, gain, ids, head)


def stats_kernel(n, planes, x_ref, out_ref, send_sem, recv_sem, local_sem):
    me = lax.axis_index("seq")
    greet([(me + d) % n for d in range(1, n)])
    lanes = n // planes
    share = x_ref.shape[1] // n

    def block(owner):
        place = (owner % lanes) * planes + owner // lanes
        return x_ref.at[:, pl.ds(pl.multiple_of(place * share // 128 * 128, 128), 128)]

    sent = []
    for d in range(1, n):
        target = (me + d) % n
        copy = pltpu.make_async_remote_copy(
            src_ref=block(target),
            dst_ref=out_ref.at[me],
            send_sem=send_sem.at[d],
            recv_sem=recv_sem.at[me],
            device_id={"seq": target},
            device_id_type=MESH,
        )
        copy.start()
        sent.append(copy)
    local = pltpu.make_async_copy(block(me), out_ref.at[me], local_sem)
    local.start()
    for d in range(1, n):
        source = (me + d) % n
        pltpu.make_async_remote_copy(
            src_ref=out_ref.at[source],
            dst_ref=out_ref.at[source],
            send_sem=send_sem.at[d],
            recv_sem=recv_sem.at[source],
            device_id={"seq": source},
            device_id_type=MESH,
        ).wait_recv()
    for copy in sent:
        copy.wait_send()
    local.wait()


def stats_exchange(n, planes, x):
    dma = pltpu.SemaphoreType.DMA
    return pl.pallas_call(
        functools.partial(stats_kernel, n, planes),
        out_shape=jax.ShapeDtypeStruct((n, x.shape[0], 128), x.dtype),
        in_specs=[pl.BlockSpec(memory_space=VMEM)],
        out_specs=pl.BlockSpec(memory_space=VMEM),
        scratch_shapes=[dma((n,)), dma((n,)), dma],
        compiler_params=pltpu.CompilerParams(collective_id=3, has_side_effects=True),
        name="stats",
    )(x)


def per_device(
    n,
    cont_query,
    cont_key,
    cont_value,
    prefix_key,
    prefix_value,
    out_weight,
    norm_gain,
    lm_head,
    target_ids,
    cont_len,
    prompt_len,
    group_of,
    rewards,
):
    cont_count, cont_span, query_width = cont_query.shape
    own_rows = cont_count * cont_span
    planes = cont_key.shape[2] // HD
    lanes = n // planes
    total_rows = own_rows * n
    device_index = lax.axis_index("seq")
    lane = device_index % lanes

    meta = jnp.zeros((8, 128), jnp.float32)
    meta = meta.at[0, :own_rows].set(target_ids.reshape(own_rows).astype(jnp.float32))
    meta = meta.at[1, :cont_count].set(rewards)
    q, ck, cv, pk, pv, meta = exchange(
        n, planes, cont_query, cont_key, cont_value, prefix_key, prefix_value, meta
    )

    def by_lane(x):
        return jnp.swapaxes(x.reshape((planes, lanes) + x.shape[1:]), 0, 1)

    lane_groups = lax.dynamic_index_in_dim(
        by_lane(group_of.reshape(n, cont_count)), lane, 0, keepdims=False
    ).reshape(planes * cont_count)
    attended = attention(lane_groups, prompt_len, q, ck, cv, pk, pv)
    tokens = gather(
        tokens_kernel, n, planes, attended, (total_rows, query_width), 1, "tokens"
    )
    hidden_cols = lax.dot_general(
        out_weight, tokens, (((0,), (1,)), ((), ())), preferred_element_type=jnp.float32
    ).astype(jnp.bfloat16)
    ids = by_lane(meta[:, 0, :own_rows]).reshape(1, total_rows).astype(jnp.int32)
    offset = (device_index * lm_head.shape[1]).astype(jnp.int32).reshape(1)
    stats = scores(n, planes, hidden_cols, norm_gain[:, None], ids, lm_head.T, offset)
    place = lane * planes + device_index // lanes
    shares = lax.dynamic_slice_in_dim(
        stats_exchange(n, planes, stats), place * own_rows % 128, own_rows, axis=2
    )
    maximum = jnp.max(shares[:, 0], axis=0)
    total_mass = jnp.sum(shares[:, 1] * jnp.exp(shares[:, 0] - maximum[None, :]), axis=0)
    picked = jnp.sum(shares[:, 2], axis=0)
    logprob = (picked - maximum - jnp.log(total_mass)).reshape(cont_count, cont_span)
    position = jnp.arange(cont_span, dtype=jnp.int32)
    live = position[None, :] < cont_len[:, None]
    token_logprob = jnp.where(live, logprob, 0.0)

    every_reward = meta[:, 1, :cont_count].reshape(n * cont_count)
    own_groups = lax.dynamic_slice_in_dim(group_of, device_index * cont_count, cont_count)
    same = (own_groups[:, None] == group_of[None, :]).astype(jnp.float32)
    group_mean = jnp.sum(same * every_reward[None, :], axis=1) / GROUP
    deviation = every_reward[None, :] - group_mean[:, None]
    spread = jnp.sqrt(jnp.sum(same * deviation * deviation, axis=1) / (GROUP - 1))
    advantage = (rewards - group_mean) / jnp.maximum(spread, REWARD_FLOOR)
    objective = advantage * jnp.sum(token_logprob, axis=1) / cont_len.astype(jnp.float32)
    return (token_logprob, advantage, objective)


def solution(mesh):
    placed = (
        P(("grp", "seq"), None, None),
        P(("grp", "seq"), None, None),
        P(("grp", "seq"), None, None),
        P("grp", "seq", None),
        P("grp", "seq", None),
        P(None, "seq"),
        P(),
        P(None, "seq"),
        P(("grp", "seq"), None),
        P(("grp", "seq")),
        P("grp"),
        P("grp"),
        P(("grp", "seq")),
    )
    return jax.shard_map(
        functools.partial(per_device, mesh.shape["seq"]),
        mesh=mesh,
        in_specs=placed,
        out_specs=(P(("grp", "seq"), None), P(("grp", "seq")), P(("grp", "seq"))),
        check_vma=False,
    )
```

```python
import functools

import jax
import jax.numpy as jnp
from jax import lax
from jax.experimental import pallas as pl
from jax.experimental.pallas import tpu as pltpu
from jax.sharding import PartitionSpec as P

HD = 128
GROUP = 16
NEGATIVE = -1e30
EPSILON = 1e-06
REWARD_FLOOR = 0.25
MESH = pl.DeviceIdType.MESH
VMEM = pltpu.VMEM
LIMIT = 60 * 1024 * 1024


class Place:
    def __init__(self, n, planes):
        self.n, self.planes = n, planes
        self.lanes = n // planes
        self.half = self.lanes // 2
        self.me = lax.axis_index("seq")
        self.plane = self.me // self.lanes
        lane = self.me % self.lanes
        self.row = lane // 2
        self.core = lane % 2

    def device(self, plane, row, core):
        return plane * self.lanes + row * 2 + core

    def plane_at(self, step):
        return (self.plane + step) % self.planes

    def row_at(self, step):
        return (self.row + step) % self.half

    def peers(self):
        out = [self.device(self.plane_at(d), self.row, self.core) for d in range(1, self.planes)]
        out += [self.device(self.plane, self.row_at(e), self.core) for e in range(1, self.half)]
        return out + [self.device(self.plane, self.row, 1 - self.core)]


def greet(peers):
    barrier = pltpu.get_barrier_semaphore()
    for peer in peers:
        pl.semaphore_signal(barrier, inc=1, device_id={"seq": peer}, device_id_type=MESH)
    pl.semaphore_wait(barrier, len(peers))


def send_count(n, planes):
    half = n // planes // 2
    return (planes - 1) + half + (planes - 1) * half + planes * (half - 1)


class Spread:
    def __init__(self, at, parts, own, full, send_sem, recv_sem, local_sem, ring=True):
        self.ring = ring
        self.at, self.parts, self.own, self.full = at, parts, own, full
        self.send_sem, self.recv_sem, self.local_sem = send_sem, recv_sem, local_sem
        self.sent = []

    def send(self, src_ref, source, part, target):
        copy = pltpu.make_async_remote_copy(
            src_ref=src_ref,
            dst_ref=self.full(source, part),
            send_sem=self.send_sem.at[len(self.sent)],
            recv_sem=self.recv_sem.at[source * self.parts + part],
            device_id={"seq": target},
            device_id_type=MESH,
        )
        copy.start()
        self.sent.append(part)

    def arrived(self, source, part):
        pltpu.make_async_remote_copy(
            src_ref=self.full(source, part),
            dst_ref=self.full(source, part),
            send_sem=self.send_sem.at[0],
            recv_sem=self.recv_sem.at[source * self.parts + part],
            device_id={"seq": self.at.device(self.at.plane, self.at.row, 1 - self.at.core)},
            device_id_type=MESH,
        ).wait_recv()

    def to_rows(self, src_ref, source, part):
        at = self.at
        for e in range(1, at.half):
            self.send(src_ref, source, part, at.device(at.plane, at.row_at(e), at.core))

    def to_core(self, src_ref, source, part):
        at = self.at
        self.send(src_ref, source, part, at.device(at.plane, at.row, 1 - at.core))

    def start(self):
        for part in range(self.parts):
            self.start_part(part)

    def start_part(self, part):
        at = self.at
        for d in range(1, 2 if self.ring else at.planes):
            target = at.plane_at(d)
            self.send(self.own(part, target), at.me, part, at.device(target, at.row, at.core))
        self.to_rows(self.own(part, at.plane), at.me, part)
        self.to_core(self.own(part, at.plane), at.me, part)
        self.keep(part).start()

    def keep(self, part):
        at = self.at
        return pltpu.make_async_copy(
            self.own(part, at.plane), self.full(at.me, part), self.local_sem.at[part]
        )

    def from_rows(self, plane, part):
        at = self.at
        for e in range(1, at.half):
            source = at.device(plane, at.row_at(e), at.core)
            self.arrived(source, part)
            self.to_core(self.full(source, part), source, part)

    def from_plane(self, step, part):
        at = self.at
        source = at.device(at.plane_at(step), at.row, at.core)
        self.arrived(source, part)
        if self.ring and step > 1:
            target = at.device(at.plane_at(1), at.row, at.core)
            self.send(self.full(source, part), source, part, target)
        self.to_rows(self.full(source, part), source, part)
        self.to_core(self.full(source, part), source, part)

    def events(self, part):
        at = self.at
        steps = [1, at.planes - 1] + list(range(2, at.planes - 1))
        if self.ring:
            steps = list(range(at.planes - 1, 0, -1))
        listed = [functools.partial(self.from_rows, at.plane, part)]
        for i, step in enumerate(steps):
            listed.append(functools.partial(self.from_plane, step, part))
            if i >= 1:
                listed.append(functools.partial(self.from_rows, at.plane_at(steps[i - 1]), part))
        listed.append(functools.partial(self.from_rows, at.plane_at(steps[-1]), part))
        return listed

    def from_core(self, part):
        at = self.at
        for plane in range(at.planes):
            for row in range(at.half):
                self.arrived(at.device(plane, row, 1 - at.core), part)

    def drain(self):
        at = self.at
        for i, part in enumerate(self.sent):
            pltpu.make_async_remote_copy(
                src_ref=self.full(at.me, part),
                dst_ref=self.full(at.me, part),
                send_sem=self.send_sem.at[i],
                recv_sem=self.recv_sem.at[0],
                device_id={"seq": at.device(at.plane, at.row, 1 - at.core)},
                device_id_type=MESH,
            ).wait_send()

    def finish(self):
        for both in zip(*[self.events(part) for part in range(self.parts)]):
            for event in both:
                event()
        for part in range(self.parts):
            self.from_core(part)
        self.drain()
        for part in range(self.parts):
            self.keep(part).wait()


def exchange_kernel(
    n,
    planes,
    q_ref,
    ck_ref,
    cv_ref,
    pk_ref,
    pv_ref,
    meta_ref,
    q_out,
    ck_out,
    cv_out,
    pk_out,
    pv_out,
    meta_out,
    send_sem,
    recv_sem,
    local_sem,
    lane_send,
    lane_recv,
    lane_local,
    meta_send,
    meta_recv,
    meta_local,
):
    at = Place(n, planes)
    greet([(at.me + d) % n for d in range(1, n)])
    conts = q_ref.shape[0]
    span = pk_ref.shape[1]

    def head(ref, plane):
        width = ref.shape[2] // planes
        return ref.at[:, :, pl.ds(pl.multiple_of(plane * width, 128), width)]

    def own(part, plane):
        return head((pk_ref, pv_ref)[part], plane)

    def full(source, part):
        start = pl.multiple_of(source * span, 128)
        return (pk_out, pv_out)[part].at[:, pl.ds(start, span), :]

    spread = Spread(at, 2, own, full, send_sem, recv_sem, local_sem, ring=False)
    spread.start()
    pairs = ((q_ref, q_out), (ck_ref, ck_out), (cv_ref, cv_out))
    waits = []
    for i, (src, dst) in enumerate(pairs):
        mine = dst.at[pl.ds(at.plane * conts, conts)]
        for d in range(1, planes):
            target = at.plane_at(d)
            copy = pltpu.make_async_remote_copy(
                src_ref=head(src, target),
                dst_ref=mine,
                send_sem=lane_send.at[i * planes + d],
                recv_sem=lane_recv.at[i * planes + at.plane],
                device_id={"seq": at.device(target, at.row, at.core)},
                device_id_type=MESH,
            )
            copy.start()
            waits.append(copy.wait_send)
        copy = pltpu.make_async_copy(head(src, at.plane), mine, lane_local.at[i])
        copy.start()
        waits.append(copy.wait)
    for d in range(1, n):
        copy = pltpu.make_async_remote_copy(
            src_ref=meta_ref,
            dst_ref=meta_out.at[at.me],
            send_sem=meta_send.at[d],
            recv_sem=meta_recv.at[at.me],
            device_id={"seq": (at.me + d) % n},
            device_id_type=MESH,
        )
        copy.start()
        waits.append(copy.wait_send)
    copy = pltpu.make_async_copy(meta_ref, meta_out.at[at.me], meta_local)
    copy.start()
    waits.append(copy.wait)
    spread.finish()
    for i, (src, dst) in enumerate(pairs):
        for d in range(1, planes):
            source = at.plane_at(d)
            landed = dst.at[pl.ds(source * conts, conts)]
            pltpu.make_async_remote_copy(
                src_ref=landed,
                dst_ref=landed,
                send_sem=lane_send.at[i * planes + d],
                recv_sem=lane_recv.at[i * planes + source],
                device_id={"seq": at.device(source, at.row, at.core)},
                device_id_type=MESH,
            ).wait_recv()
    for d in range(1, n):
        source = (at.me + d) % n
        pltpu.make_async_remote_copy(
            src_ref=meta_ref,
            dst_ref=meta_out.at[source],
            send_sem=meta_send.at[d],
            recv_sem=meta_recv.at[source],
            device_id={"seq": source},
            device_id_type=MESH,
        ).wait_recv()
    for wait in waits:
        wait()


def exchange(n, planes, q, ck, cv, pk, pv, meta):
    conts, steps, width = q.shape
    prompts, span, _ = pk.shape
    dma = pltpu.SemaphoreType.DMA
    shape = jax.ShapeDtypeStruct
    return pl.pallas_call(
        functools.partial(exchange_kernel, n, planes),
        out_shape=(
            shape((conts * planes, steps, width // planes), q.dtype),
            shape((conts * planes, steps, ck.shape[2] // planes), q.dtype),
            shape((conts * planes, steps, ck.shape[2] // planes), q.dtype),
            shape((prompts, span * n, pk.shape[2] // planes), q.dtype),
            shape((prompts, span * n, pk.shape[2] // planes), q.dtype),
            shape((n,) + meta.shape, meta.dtype),
        ),
        in_specs=[pl.BlockSpec(memory_space=VMEM)] * 6,
        out_specs=(pl.BlockSpec(memory_space=VMEM),) * 6,
        scratch_shapes=[
            dma((2 * send_count(n, planes),)),
            dma((2 * n,)),
            dma((2,)),
            dma((3 * planes,)),
            dma((3 * planes,)),
            dma((3,)),
            dma((n,)),
            dma((n,)),
            dma,
        ],
        compiler_params=pltpu.CompilerParams(
            collective_id=0, has_side_effects=True, vmem_limit_bytes=LIMIT
        ),
        name="exchange",
    )(q, ck, cv, pk, pv, meta)


def attention_kernel(group_ref, length_ref, q_ref, ck_ref, cv_ref, pk_ref, pv_ref, out_ref):
    cont = pl.program_id(0)
    prompt = group_ref[cont]
    length = length_ref[prompt]
    steps, width = q_ref.shape[1:]
    heads = width // HD
    q = q_ref[0]
    rows = jnp.concatenate([q[:, h * HD : (h + 1) * HD] for h in range(heads)], axis=0)
    contract = (((1,), (1,)), ((), ()))
    early = lax.dot_general(rows, pk_ref[prompt], contract, preferred_element_type=jnp.float32)
    late = lax.dot_general(rows, ck_ref[0], contract, preferred_element_type=jnp.float32)
    scale = HD ** (-0.5)
    column = lax.broadcasted_iota(jnp.int32, early.shape, 1)
    early = jnp.where(column < length, early * scale, NEGATIVE)
    line = lax.broadcasted_iota(jnp.int32, late.shape, 0) % steps
    late = jnp.where(
        lax.broadcasted_iota(jnp.int32, late.shape, 1) <= line, late * scale, NEGATIVE
    )
    peak = jnp.maximum(
        jnp.max(early, axis=1, keepdims=True), jnp.max(late, axis=1, keepdims=True)
    )
    early = jnp.exp(early - peak).astype(jnp.bfloat16)
    late = jnp.exp(late - peak).astype(jnp.bfloat16)
    total = jnp.sum(early.astype(jnp.float32), axis=1, keepdims=True) + jnp.sum(
        late.astype(jnp.float32), axis=1, keepdims=True
    )
    mixed = jnp.dot(early, pv_ref[prompt], preferred_element_type=jnp.float32) + jnp.dot(
        late, cv_ref[0], preferred_element_type=jnp.float32
    )
    mixed = (mixed / total).astype(jnp.bfloat16)
    out_ref[...] = jnp.concatenate(
        [mixed[h * steps : (h + 1) * steps] for h in range(heads)], axis=1
    )


def attention(groups, lengths, q, ck, cv, pk, pv):
    conts, steps, width = q.shape
    whole = pl.BlockSpec(memory_space=VMEM)
    scalar = pl.BlockSpec(memory_space=pltpu.SMEM)
    return pl.pallas_call(
        attention_kernel,
        out_shape=jax.ShapeDtypeStruct((conts * steps, width), jnp.bfloat16),
        grid=(conts,),
        in_specs=[
            scalar,
            scalar,
            pl.BlockSpec((1, steps, width), lambda c: (c, 0, 0)),
            pl.BlockSpec((1, steps, ck.shape[2]), lambda c: (c, 0, 0)),
            pl.BlockSpec((1, steps, ck.shape[2]), lambda c: (c, 0, 0)),
            whole,
            whole,
        ],
        out_specs=pl.BlockSpec((steps, width), lambda c: (c, 0)),
        compiler_params=pltpu.CompilerParams(vmem_limit_bytes=LIMIT),
        name="attention",
    )(groups, lengths, q, ck, cv, pk, pv)


PARTS = 2


def tokens_kernel(n, planes, x_ref, out_ref, send_sem, recv_sem, local_sem):
    at = Place(n, planes)
    greet(at.peers())
    rows, width = x_ref.shape
    piece = rows // PARTS

    def own(part, plane):
        return x_ref.at[pl.ds(part * piece, piece)]

    def full(source, part):
        start = pl.multiple_of(source % at.lanes * rows + part * piece, 16)
        column = pl.multiple_of(source // at.lanes * width, 128)
        return out_ref.at[pl.ds(start, piece), pl.ds(column, width)]

    spread = Spread(at, PARTS, own, full, send_sem, recv_sem, local_sem)
    spread.start()
    spread.finish()


def gather(kernel, n, planes, x, shape, number, name):
    dma = pltpu.SemaphoreType.DMA
    return pl.pallas_call(
        functools.partial(kernel, n, planes),
        out_shape=jax.ShapeDtypeStruct(shape, x.dtype),
        in_specs=[pl.BlockSpec(memory_space=VMEM)],
        out_specs=pl.BlockSpec(memory_space=VMEM),
        scratch_shapes=[
            dma((PARTS * send_count(n, planes),)),
            dma((PARTS * n,)),
            dma((PARTS,)),
        ],
        compiler_params=pltpu.CompilerParams(
            collective_id=number, has_side_effects=True, vmem_limit_bytes=LIMIT
        ),
        name=name,
    )(x)


TILE = 1584
SUB = 528
CUTS = 4
BAND = 256
STEP = 128


def scores_kernel(
    n,
    planes,
    offset_ref,
    x_ref,
    gain_ref,
    ids_ref,
    head_hbm,
    out_ref,
    hidden_ref,
    normed_ref,
    head_ref,
    max_ref,
    sum_ref,
    pick_ref,
    send_sem,
    recv_sem,
    local_sem,
    head_sem,
):
    at = Place(n, planes)
    greet(at.peers())
    rows, tokens = x_ref.shape
    depth = rows * n
    vocab = head_hbm.shape[0]
    piece = tokens // CUTS
    tiles, rest = vocab // TILE, vocab % TILE

    def own(part, plane):
        return x_ref.at[:, pl.ds(part * piece, piece)]

    def full(source, part):
        start = pl.multiple_of(source * rows, 16)
        return hidden_ref.at[pl.ds(start, rows), pl.ds(part * piece, piece)]

    spread = Spread(at, CUTS, own, full, send_sem, recv_sem, local_sem)
    spread.start_part(0)
    spread.start_part(1)

    def load(tile, size):
        cut = pl.ds(pl.multiple_of(tile * TILE, 8), size)
        return pltpu.make_async_copy(head_hbm.at[cut], head_ref.at[cut], head_sem.at[tile])

    for tile in range(tiles):
        load(tile, TILE).start()
    if rest:
        load(tiles, rest).start()

    max_ref[...] = jnp.full_like(max_ref, NEGATIVE)
    sum_ref[...] = jnp.zeros_like(sum_ref)
    pick_ref[...] = jnp.zeros_like(pick_ref)

    def normalize(part):
        columns = pl.ds(part * piece, piece)

        def square(i, total):
            cut = pl.ds(pl.multiple_of(i * STEP, STEP), STEP)
            wide = hidden_ref[cut, columns].astype(jnp.float32)
            return total + jnp.sum((wide * wide).reshape(STEP // 8, 8, piece), axis=0)

        total = lax.fori_loop(0, depth // STEP, square, jnp.zeros((8, piece), jnp.float32))
        factor = lax.rsqrt(jnp.sum(total, axis=0, keepdims=True) / depth + EPSILON)

        @pl.loop(0, depth // STEP)
        def _(i):
            cut = pl.ds(pl.multiple_of(i * STEP, STEP), STEP)
            wide = hidden_ref[cut, columns].astype(jnp.float32)
            normed_ref[cut] = (wide * factor * gain_ref[cut]).astype(jnp.bfloat16)

    def score(part, tile, size):
        if part == 0:
            load(tile, size).wait()
        base = tile * TILE + offset_ref[0]

        def product(start, width, band):
            at_row = pl.ds(pl.multiple_of(tile * TILE + start, 8), width)
            return jnp.dot(
                head_ref[at_row], normed_ref[:, band], preferred_element_type=jnp.float32
            )

        def absorb(start, width, band, logits):
            columns = slice(part * piece + band.start, part * piece + band.stop)
            row = start + lax.broadcasted_iota(jnp.int32, logits.shape, 0)
            chosen = jnp.where(row == ids_ref[:, columns] - base, logits, 0.0)
            split = (width // 8, 8, BAND)
            before = max_ref[:, columns]
            best = jnp.maximum(before, jnp.max(logits.reshape(split), axis=0))
            mass = jnp.sum(jnp.exp(logits.reshape(split) - best[None]), axis=0)
            max_ref[:, columns] = best
            sum_ref[:, columns] = sum_ref[:, columns] * jnp.exp(before - best) + mass
            pick_ref[:, columns] += jnp.sum(chosen.reshape(split), axis=0)

        pending = None
        for begin in range(0, piece, BAND):
            for start in range(0, size, SUB):
                job = (start, min(SUB, size - start), slice(begin, begin + BAND))
                logits = product(*job)
                if pending is not None:
                    absorb(*pending)
                pending = job + (logits,)
        absorb(*pending)

    def score_all(part, events):
        each = -(-len(events) // max(tiles, 1))

        @pl.loop(0, tiles)
        def _(tile):
            for i, event in enumerate(events):
                pl.when(tile == i // each)(event)
            score(part, tile, TILE)

        if rest:
            score(part, tiles, rest)

    listed = [spread.events(part) for part in range(CUTS)]
    rows0, za0, zb0, ya0, zc0 = listed[0][:5]
    early = [rows0, za0, zb0] + listed[1][:2] + [ya0, zc0] + listed[1][2:3]
    early += [functools.partial(spread.start_part, 2)] + listed[0][5:]
    for event in early:
        event()
    for part in range(CUTS):
        spread.from_core(part)
        spread.keep(part).wait()
        normalize(part)
        beside = []
        if part + 1 < CUTS:
            now = listed[part + 1][3:]
            after = listed[part + 2][:3] if part + 2 < CUTS else [None] * 3
            beside = [now[0], now[1], after[0], after[1], now[2], after[2]] + now[3:]
            if part + 3 < CUTS:
                beside.append(functools.partial(spread.start_part, part + 3))
        score_all(part, [event for event in beside if event is not None])
    spread.drain()
    peak = max_ref[...]
    top = jnp.max(peak, axis=0, keepdims=True)
    out_ref[...] = jnp.zeros_like(out_ref)
    out_ref[0:1] = top
    out_ref[1:2] = jnp.sum(sum_ref[...] * jnp.exp(peak - top), axis=0, keepdims=True)
    out_ref[2:3] = jnp.sum(pick_ref[...], axis=0, keepdims=True)


def scores(n, planes, x, gain, ids, head, offset):
    rows, tokens = x.shape
    depth = rows * n
    dma = pltpu.SemaphoreType.DMA
    vmem = pl.BlockSpec(memory_space=VMEM)
    running = VMEM((8, tokens), jnp.float32)
    return pl.pallas_call(
        functools.partial(scores_kernel, n, planes),
        out_shape=jax.ShapeDtypeStruct((8, tokens), jnp.float32),
        in_specs=[
            pl.BlockSpec(memory_space=pltpu.SMEM),
            vmem,
            vmem,
            vmem,
            pl.BlockSpec(memory_space=pl.ANY),
        ],
        out_specs=vmem,
        scratch_shapes=[
            VMEM((depth, tokens), x.dtype),
            VMEM((depth, tokens // CUTS), x.dtype),
            VMEM(head.shape, head.dtype),
            running,
            running,
            running,
            dma((CUTS * send_count(n, planes),)),
            dma((CUTS * n,)),
            dma((CUTS,)),
            dma((pl.cdiv(head.shape[0], TILE),)),
        ],
        compiler_params=pltpu.CompilerParams(
            collective_id=2, has_side_effects=True, vmem_limit_bytes=LIMIT
        ),
        name="scores",
    )(offset, x, gain, ids, head)


def stats_kernel(n, planes, x_ref, out_ref, send_sem, recv_sem, local_sem):
    me = lax.axis_index("seq")
    greet([(me + d) % n for d in range(1, n)])
    lanes = n // planes
    share = x_ref.shape[1] // n

    def block(owner):
        place = (owner % lanes) * planes + owner // lanes
        return x_ref.at[:, pl.ds(pl.multiple_of(place * share // 128 * 128, 128), 128)]

    sent = []
    for d in range(1, n):
        target = (me + d) % n
        copy = pltpu.make_async_remote_copy(
            src_ref=block(target),
            dst_ref=out_ref.at[me],
            send_sem=send_sem.at[d],
            recv_sem=recv_sem.at[me],
            device_id={"seq": target},
            device_id_type=MESH,
        )
        copy.start()
        sent.append(copy)
    local = pltpu.make_async_copy(block(me), out_ref.at[me], local_sem)
    local.start()
    for d in range(1, n):
        source = (me + d) % n
        pltpu.make_async_remote_copy(
            src_ref=out_ref.at[source],
            dst_ref=out_ref.at[source],
            send_sem=send_sem.at[d],
            recv_sem=recv_sem.at[source],
            device_id={"seq": source},
            device_id_type=MESH,
        ).wait_recv()
    for copy in sent:
        copy.wait_send()
    local.wait()


def stats_exchange(n, planes, x):
    dma = pltpu.SemaphoreType.DMA
    return pl.pallas_call(
        functools.partial(stats_kernel, n, planes),
        out_shape=jax.ShapeDtypeStruct((n, x.shape[0], 128), x.dtype),
        in_specs=[pl.BlockSpec(memory_space=VMEM)],
        out_specs=pl.BlockSpec(memory_space=VMEM),
        scratch_shapes=[dma((n,)), dma((n,)), dma],
        compiler_params=pltpu.CompilerParams(collective_id=3, has_side_effects=True),
        name="stats",
    )(x)


def per_device(
    n,
    cont_query,
    cont_key,
    cont_value,
    prefix_key,
    prefix_value,
    out_weight,
    norm_gain,
    lm_head,
    target_ids,
    cont_len,
    prompt_len,
    group_of,
    rewards,
):
    cont_count, cont_span, query_width = cont_query.shape
    own_rows = cont_count * cont_span
    planes = cont_key.shape[2] // HD
    lanes = n // planes
    total_rows = own_rows * n
    device_index = lax.axis_index("seq")
    lane = device_index % lanes

    meta = jnp.zeros((8, 128), jnp.float32)
    meta = meta.at[0, :own_rows].set(target_ids.reshape(own_rows).astype(jnp.float32))
    meta = meta.at[1, :cont_count].set(rewards)
    q, ck, cv, pk, pv, meta = exchange(
        n, planes, cont_query, cont_key, cont_value, prefix_key, prefix_value, meta
    )

    def by_lane(x):
        return jnp.swapaxes(x.reshape((planes, lanes) + x.shape[1:]), 0, 1)

    lane_groups = lax.dynamic_index_in_dim(
        by_lane(group_of.reshape(n, cont_count)), lane, 0, keepdims=False
    ).reshape(planes * cont_count)
    attended = attention(lane_groups, prompt_len, q, ck, cv, pk, pv)
    tokens = gather(
        tokens_kernel, n, planes, attended, (total_rows, query_width), 1, "tokens"
    )
    hidden_cols = lax.dot_general(
        out_weight, tokens, (((0,), (1,)), ((), ())), preferred_element_type=jnp.float32
    ).astype(jnp.bfloat16)
    ids = by_lane(meta[:, 0, :own_rows]).reshape(1, total_rows).astype(jnp.int32)
    offset = (device_index * lm_head.shape[1]).astype(jnp.int32).reshape(1)
    stats = scores(n, planes, hidden_cols, norm_gain[:, None], ids, lm_head.T, offset)
    place = lane * planes + device_index // lanes
    shares = lax.dynamic_slice_in_dim(
        stats_exchange(n, planes, stats), place * own_rows % 128, own_rows, axis=2
    )
    maximum = jnp.max(shares[:, 0], axis=0)
    total_mass = jnp.sum(shares[:, 1] * jnp.exp(shares[:, 0] - maximum[None, :]), axis=0)
    picked = jnp.sum(shares[:, 2], axis=0)
    logprob = (picked - maximum - jnp.log(total_mass)).reshape(cont_count, cont_span)
    position = jnp.arange(cont_span, dtype=jnp.int32)
    live = position[None, :] < cont_len[:, None]
    token_logprob = jnp.where(live, logprob, 0.0)

    every_reward = meta[:, 1, :cont_count].reshape(n * cont_count)
    own_groups = lax.dynamic_slice_in_dim(group_of, device_index * cont_count, cont_count)
    same = (own_groups[:, None] == group_of[None, :]).astype(jnp.float32)
    group_mean = jnp.sum(same * every_reward[None, :], axis=1) / GROUP
    deviation = every_reward[None, :] - group_mean[:, None]
    spread = jnp.sqrt(jnp.sum(same * deviation * deviation, axis=1) / (GROUP - 1))
    advantage = (rewards - group_mean) / jnp.maximum(spread, REWARD_FLOOR)
    objective = advantage * jnp.sum(token_logprob, axis=1) / cont_len.astype(jnp.float32)
    return (token_logprob, advantage, objective)


def solution(mesh):
    placed = (
        P(("grp", "seq"), None, None),
        P(("grp", "seq"), None, None),
        P(("grp", "seq"), None, None),
        P("grp", "seq", None),
        P("grp", "seq", None),
        P(None, "seq"),
        P(),
        P(None, "seq"),
        P(("grp", "seq"), None),
        P(("grp", "seq")),
        P("grp"),
        P("grp"),
        P(("grp", "seq")),
    )
    return jax.shard_map(
        functools.partial(per_device, mesh.shape["seq"]),
        mesh=mesh,
        in_specs=placed,
        out_specs=(P(("grp", "seq"), None), P(("grp", "seq")), P(("grp", "seq"))),
        check_vma=False,
    )
```
